32 devices in a mesh: row: 4 (over y, x), col: 4 (over z), depth: 2 (over core).
Axes of the slice: x: 2, y: 2, z: 4, core: 2. Of those that a mesh axis runs over, the one named last changes fastest.
Arguments:
- halves: bfloat16 [2, 8192, 16384], P(None, 'row', ('col', 'depth')), may hold values from -6 to 6
- spectrum: float32 [2, 16384], P(None, ('col', 'depth')), as said below
- wanted: int32 [4096], P('col'), may hold values from 0 to 32766, as said below
- fraction: float32 [4096], P('col'), may hold values from 0.05 to 0.95
Outputs:
- eigvec: float32 [2, 8192, 4096], P(None, 'row', ('col', 'depth'))
The draws below stay inside these ranges and needn't reach their ends.
Inputs may be any that keep to these rules, and one draw needn't show every extreme that they name: Read in the order spectrum[0,0], spectrum[1,0], spectrum[0,1], spectrum[1,1], ... the values rise strictly, each by more than 0.05 over the one before. `wanted`: distinct positions in that merged order of the 32768 eigenvalues.
All inputs are finite; a program needn't handle non-finite values.
Results may differ from the reference program's by a relative error of at most 0.0029.
Values may be sent and summed in bfloat16 or wider, within the bound.
A program may use at most 192 MiB of HBM per device.

```python
import math
import jax
import jax.numpy as jnp
from jax import lax

H = 16384
R = 8192
K = 4096


def draw_halves(key, part):
    noise_key = jax.random.fold_in(key, 11)
    random_part = jnp.clip(jax.random.normal(noise_key, (2, R, H), jnp.float32), -6.0, 6.0)
    values = random_part
    return values.astype(jnp.bfloat16)


def draw_spectrum(key, part):
    gaps = jnp.exp(jax.random.uniform(key, (2 * H,), jnp.float32, math.log(0.5), math.log(2.0)))
    ordered = jnp.cumsum(gaps)
    ordered = ordered - 0.5 * ordered[-1]
    return ordered.reshape(H, 2).T.astype(jnp.float32)


def draw_wanted(key, part):
    return jax.random.permutation(key, 2 * H - 1)[:K].astype(jnp.int32)


def level_of(key, extent, pieces, low, top_value):
    gain = 1.0
    for position, blocks in pieces:
        draws = jax.random.uniform(jax.random.fold_in(jax.random.fold_in(key, 6), position), (blocks,), jnp.float32, low / len(pieces), top_value / len(pieces))
        gain = gain * jnp.repeat(jnp.exp(draws), extent[position] // blocks).reshape((-1,) + (1,) * (len(extent) - 1 - position))
    return gain


def setup_inputs(seed: int = 0) -> dict:
    arg_keys = jax.random.split(jax.random.key(seed), 5)
    return {
        "halves": draw_halves(jax.random.fold_in(arg_keys[4], 71), 0),
        "spectrum": draw_spectrum(jax.random.fold_in(arg_keys[4], 71), 0),
        "wanted": draw_wanted(jax.random.fold_in(arg_keys[4], 71), 0),
        "fraction": jnp.clip(0.05 + 0.9 * jax.random.uniform(arg_keys[3], (K,), jnp.float32) ** level_of(arg_keys[3], (K,), ((0, 4),), -0.2, 0.2), 0.05, 0.95),
    }


def root_terms(spectrum, wanted):
    ordered = jnp.stack([spectrum[0], spectrum[1]], axis=1).reshape(-1)
    lower = jnp.take(ordered, wanted)
    upper = jnp.take(ordered, wanted + 1)
    return (lower, upper - lower)

def reference(halves, spectrum, wanted, fraction):
    seam = jnp.stack([halves[0, R - 1], halves[1, 0]]).astype(jnp.float32)
    lower, width = root_terms(spectrum, wanted)
    block = math.gcd(K, 512)
    count = K // block

    def one(index):
        start = (index * block).astype(jnp.int32)
        low = lax.dynamic_slice_in_dim(lower, start, block)
        wid = lax.dynamic_slice_in_dim(width, start, block)
        frc = lax.dynamic_slice_in_dim(fraction, start, block)
        cauchy = seam[:, :, None] / (spectrum[:, :, None] - low[None, None, :] - frc[None, None, :] * wid[None, None, :])
        norms = jnp.sqrt(lax.optimization_barrier(jnp.sum(cauchy * cauchy, axis=(0, 1))))
        rounded = cauchy.astype(jnp.bfloat16)
        first = jnp.dot(halves[0], rounded[0], preferred_element_type=jnp.float32)
        second = jnp.dot(halves[1], rounded[1], preferred_element_type=jnp.float32)
        return jnp.stack([first, second]) / norms[None, None, :]
    result = lax.map(one, jnp.arange(count).astype(jnp.int32))
    return jnp.transpose(result, (1, 2, 0, 3)).reshape(2, R, K)
```

```python
import functools
import math

import jax
import jax.numpy as jnp
from jax import lax
from jax.experimental import pallas as pl
from jax.experimental.pallas import tpu as pltpu
from jax.sharding import PartitionSpec as P


def product_kernel(own_ref, par_ref, roots_ref, line_ref, out_ref, block_ref):
    inner = block_ref.shape[0]
    half = inner // 2
    step = math.gcd(inner, 64)

    @pl.when(pl.program_id(0) == 0)
    def _():
        lower = roots_ref[0:1, :]
        shift = roots_ref[1:2, :]

        def one(i, carry):
            rows = pl.ds(pl.multiple_of(i * step, step), step)
            value = line_ref[rows, 0:1]
            seam = line_ref[rows, 1:2]
            gap = (value - lower) - shift
            guess = pl.reciprocal(gap, approx=True)
            inverse = guess + guess * (1.0 - gap * guess)
            block_ref[rows, :] = (seam * inverse).astype(jnp.bfloat16)
            return carry

        lax.fori_loop(0, inner // step, one, 0)

    first = jnp.dot(own_ref[...], block_ref[0:half, :], preferred_element_type=jnp.float32)
    second = jnp.dot(par_ref[...], block_ref[half:inner, :], preferred_element_type=jnp.float32)
    out_ref[...] = (first + second).astype(out_ref.dtype)


def product(side, own, partner, roots, lines, dtype):
    rows = own.shape[1]
    half = own.shape[2]
    cols = roots.shape[1]
    tile = math.gcd(rows, 256)
    return pl.pallas_call(
        product_kernel,
        grid=(rows // tile,),
        in_specs=[
            pl.BlockSpec((None, tile, half), lambda i: (side, i, 0)),
            pl.BlockSpec((None, tile, half), lambda i: (side, i, 0)),
            pl.BlockSpec((2, cols), lambda i: (0, 0)),
            pl.BlockSpec((None, 2 * half, 2), lambda i: (side, 0, 0)),
        ],
        out_specs=pl.BlockSpec((tile, cols), lambda i: (i, 0)),
        out_shape=jax.ShapeDtypeStruct((rows, cols), dtype),
        scratch_shapes=[pltpu.VMEM((2 * half, cols), jnp.bfloat16)],
        cost_estimate=pl.CostEstimate(
            flops=4 * rows * half * cols,
            bytes_accessed=4 * rows * half + 4 * rows * cols,
            transcendentals=2 * half * cols,
        ),
        compiler_params=pltpu.CompilerParams(dimension_semantics=("arbitrary",)),
    )(own, partner, roots, lines)


def combine_kernel(count, *refs):
    own_ref = refs[0]
    norm_ref = refs[1 + count]
    out_ref = refs[-1]
    total = own_ref[...]
    for k in range(count):
        total = total + refs[1 + k][...].astype(jnp.float32)
    out_ref[...] = total / norm_ref[...]


def combine(side, own, parts, norms, whole):
    rows, cols = own.shape
    tile = math.gcd(rows, 256)
    count = len(parts)
    block = pl.BlockSpec((tile, cols), lambda i: (i, 0))
    operands = [own, *parts, norms]
    in_specs = [block] * (1 + count) + [pl.BlockSpec((1, cols), lambda i: (0, 0))]
    aliases = {}
    if whole is not None:
        aliases = {len(operands): 0}
        operands.append(whole)
        in_specs.append(pl.BlockSpec(memory_space=pl.ANY))
    return pl.pallas_call(
        functools.partial(combine_kernel, count),
        grid=(rows // tile,),
        in_specs=in_specs,
        out_specs=pl.BlockSpec((None, tile, cols), lambda i: (side, i, 0)),
        out_shape=jax.ShapeDtypeStruct((2, rows, cols), jnp.float32),
        input_output_aliases=aliases,
        cost_estimate=pl.CostEstimate(
            flops=(2 + count) * rows * cols, bytes_accessed=(8 + 2 * count) * rows * cols, transcendentals=0
        ),
        compiler_params=pltpu.CompilerParams(dimension_semantics=("arbitrary",)),
    )(*operands)


MESH = pl.DeviceIdType.MESH
SLOTS = 10
SENDS = 3
LAG = 3
BLOCKS = 8


def line_kernel(n, halves, roots, lines, out, norm, own, par, cauchy, total, got, send, square, squares,
                own_sem, par_send, par_got, send_sem, got_sem, square_send, square_got, free):
    c = lax.axis_index("col")
    d = lax.axis_index("depth")
    inner = cauchy.shape[1]
    half = inner // 2
    rows = own.shape[1]
    tile = rows // BLOCKS
    chunks = 2 * BLOCKS
    step = math.gcd(inner, 64)

    def part(b):
        return b // BLOCKS, pl.ds(pl.multiple_of((b % BLOCKS) * tile, tile), tile)

    def own_copy(b):
        side, where = part(b)
        return pltpu.make_async_copy(halves.at[side, where], own.at[side, where], own_sem.at[b])

    def par_copy(b):
        side, where = part(b)
        return pltpu.make_async_remote_copy(
            src_ref=halves.at[side, where],
            dst_ref=par.at[side, where],
            send_sem=par_send.at[b],
            recv_sem=par_got.at[b],
            device_id={"depth": 1 - d},
            device_id_type=MESH,
        )

    def square_copy(source, target):
        return pltpu.make_async_remote_copy(
            src_ref=square.at[target],
            dst_ref=squares.at[source],
            send_sem=square_send.at[target],
            recv_sem=square_got.at[source],
            device_id={"col": target},
            device_id_type=MESH,
        )

    def each(count, act):
        def one(b, carry):
            act(b)
            return carry

        lax.fori_loop(0, count, one, 0)

    each(chunks, lambda b: own_copy(b).start())

    barrier = pltpu.get_barrier_semaphore()
    pl.semaphore_signal(barrier, inc=1, device_id={"depth": 1 - d}, device_id_type=MESH)
    for k in range(1, n):
        pl.semaphore_signal(barrier, inc=1, device_id={"col": (c + k) % n}, device_id_type=MESH)
    pl.semaphore_wait(barrier, n)

    each(chunks, lambda b: par_copy(b).start())

    def item(q, carry):
        s = q // 2
        way = q % 2
        far = c + way * (n - 1 - 2 * c)
        t = s - LAG * far
        u = t // chunks
        i = t - u * chunks
        side, where = part(i)
        mark = n - 1 - u
        target = mark + way * (n - 1 - 2 * mark)
        valid = (t >= 0) & (t < jnp.minimum(n - far, n - 1) * chunks)
        forward = valid & (mark > far)
        arrive = valid & (mark == far)
        first = arrive & (2 * far > n - 1)
        later = arrive & (2 * far <= n - 1)
        dot = forward | first
        incoming = valid & (far > 0)
        slot = t % SLOTS
        spot = t % SENDS
        ahead = c + 1 - 2 * way
        behind = c - 1 + 2 * way

        def line_copy(at):
            return pltpu.make_async_remote_copy(
                src_ref=send.at[way, at % SENDS],
                dst_ref=got.at[way, at % SLOTS],
                send_sem=send_sem.at[way, at % SENDS],
                recv_sem=got_sem.at[way, at % SLOTS],
                device_id={"col": ahead},
                device_id_type=MESH,
            )

        @pl.when((way == 0) & (s < chunks))
        def _():
            own_copy(s).wait()
            par_copy(s).wait_recv()

        @pl.when(dot & (i % BLOCKS == 0))
        def _():
            lower = roots[target, 0:1, :]
            shift = roots[target, 1:2, :]

            def one(k, tally):
                at = pl.ds(pl.multiple_of(k * step, step), step)
                value = lines[side, at, 0:1]
                seam = lines[side, at, 1:2]
                gap = (value - lower) - shift
                guess = pl.reciprocal(gap, approx=True)
                inverse = guess + guess * (1.0 - gap * guess)
                terms = seam * inverse
                cauchy[way, at, :] = terms.astype(jnp.bfloat16)
                terms = terms * terms
                for j in range(step // 8):
                    tally = tally + terms[8 * j : 8 * j + 8, :]
                return tally

            tally = lax.fori_loop(0, inner // step, one, jnp.zeros(square.shape[1:], jnp.float32))

            @pl.when(side == 0)
            def _():
                square[target] = tally

            @pl.when(side == 1)
            def _():
                square[target] = square[target] + tally

            @pl.when((side == 1) & forward)
            def _():
                square_copy(c, target).start()

        @pl.when(dot)
        def _():
            a = jnp.dot(own[side, where, :], cauchy[way, 0:half, :], preferred_element_type=jnp.float32)
            b = jnp.dot(par[side, where, :], cauchy[way, half:inner, :], preferred_element_type=jnp.float32)
            total[...] = a + b

        @pl.when(incoming)
        def _():
            line_copy(t).wait_recv()

        @pl.when(forward)
        def _():
            @pl.when(t >= SENDS)
            def _():
                line_copy(t - SENDS).wait_send()

        @pl.when(forward & (far == 0))
        def _():
            send[way, spot] = total[...].astype(jnp.bfloat16)

        @pl.when(forward & (far > 0))
        def _():
            send[way, spot] = (total[...] + got[way, slot].astype(jnp.float32)).astype(jnp.bfloat16)

        @pl.when(first)
        def _():
            out[side, where, :] = total[...] + got[way, slot].astype(jnp.float32)

        @pl.when(later)
        def _():
            out[side, where, :] = out[side, where, :] + got[way, slot].astype(jnp.float32)

        @pl.when(incoming & (t + SLOTS < (n - far) * chunks))
        def _():
            pl.semaphore_signal(free.at[way], inc=1, device_id={"col": behind}, device_id_type=MESH)

        @pl.when(forward)
        def _():
            @pl.when(t >= SLOTS)
            def _():
                pl.semaphore_wait(free.at[way], 1)

            line_copy(t).start()

        return carry

    steps = (n - 1) * (chunks + LAG)
    lax.fori_loop(0, 2 * steps, item, 0)

    for way in range(2):
        far = c + way * (n - 1 - 2 * c)

        @pl.when(far < n - 1)
        def _():
            for spot in range(SENDS):
                pltpu.make_async_remote_copy(
                    src_ref=send.at[way, spot],
                    dst_ref=got.at[way, spot],
                    send_sem=send_sem.at[way, spot],
                    recv_sem=got_sem.at[way, spot],
                    device_id={"col": c + 1 - 2 * way},
                    device_id_type=MESH,
                ).wait_send()

    each(chunks, lambda b: par_copy(b).wait_send())
    sums = square[c]
    for k in range(1, n):
        other = (c + k) % n
        square_copy(c, other).wait_send()
        square_copy(other, c).wait_recv()
        sums = sums + squares[other]
    norm[...] = jnp.sqrt(jnp.sum(sums, axis=0, keepdims=True))


def line_product(n, halves, roots, lines):
    _, rows, half = halves.shape
    cols = roots.shape[2]
    tile = rows // BLOCKS
    chunks = 2 * BLOCKS
    dma = pltpu.SemaphoreType.DMA
    return pl.pallas_call(
        functools.partial(line_kernel, n),
        in_specs=[
            pl.BlockSpec(memory_space=pl.ANY),
            pl.BlockSpec(memory_space=pltpu.VMEM),
            pl.BlockSpec(memory_space=pltpu.VMEM),
        ],
        out_specs=[pl.BlockSpec(memory_space=pltpu.VMEM), pl.BlockSpec(memory_space=pltpu.VMEM)],
        out_shape=[
            jax.ShapeDtypeStruct((2, rows, cols), jnp.float32),
            jax.ShapeDtypeStruct((1, cols), jnp.float32),
        ],
        scratch_shapes=[
            pltpu.VMEM((2, rows, half), jnp.bfloat16),
            pltpu.VMEM((2, rows, half), jnp.bfloat16),
            pltpu.VMEM((2, 2 * half, cols), jnp.bfloat16),
            pltpu.VMEM((tile, cols), jnp.float32),
            pltpu.VMEM((2, SLOTS, tile, cols), jnp.bfloat16),
            pltpu.VMEM((2, SENDS, tile, cols), jnp.bfloat16),
            pltpu.VMEM((n, 8, cols), jnp.float32),
            pltpu.VMEM((n, 8, cols), jnp.float32),
            dma((chunks,)),
            dma((chunks,)),
            dma((chunks,)),
            dma((2, SENDS)),
            dma((2, SLOTS)),
            dma((n,)),
            dma((n,)),
            pltpu.SemaphoreType.REGULAR((2,)),
        ],
        cost_estimate=pl.CostEstimate(
            flops=8 * n * rows * half * cols,
            bytes_accessed=8 * rows * half + 8 * rows * cols,
            transcendentals=4 * n * half * cols,
        ),
        compiler_params=pltpu.CompilerParams(
            collective_id=0, has_side_effects=True, vmem_limit_bytes=67043328
        ),
    )(halves, roots, lines)


def look_up(table, row, lane):
    pick = (row[:, None] == lax.broadcasted_iota(jnp.int32, (1, table.shape[0]), 1)).astype(jnp.float32)
    lines = jnp.dot(pick, table, precision=lax.Precision.HIGHEST, preferred_element_type=jnp.float32)
    lanes = lax.broadcasted_iota(jnp.int32, (1, table.shape[1]), 1)
    return jnp.sum(jnp.where(lane[:, None] == lanes, lines, 0.0), axis=1)


def body(halves, spectrum, wanted, fraction):
    ncols = lax.axis_size("col")
    ndepth = lax.axis_size("depth")
    nrow = lax.axis_size("row")
    col = lax.axis_index("col")
    layer = lax.axis_index("depth")
    rows_here = halves.shape[1]
    width_here = halves.shape[2]
    kcol = wanted.shape[0]
    share = kcol // ndepth

    edges = jnp.stack([halves[0, rows_here - 1], halves[1, 0]])
    edges = lax.all_gather(edges, "row", axis=0, tiled=False)
    seam = jnp.stack([edges[nrow - 1, 0], edges[0, 1]]).astype(jnp.float32)

    lanes = math.gcd(width_here, 128)
    flat = jnp.concatenate(
        [spectrum.reshape(-1), seam.reshape(-1), wanted.astype(jnp.float32), fraction]
    )
    flat = lax.all_gather(flat, ("col", "depth"), axis=0, tiled=False)
    pieces = jnp.split(flat, [2 * width_here, 4 * width_here, 4 * width_here + kcol], axis=1)
    values, seams, position, frac = pieces
    table = values.reshape(-1, lanes)
    position = position.reshape(ncols, ndepth, kcol)[:, 0]
    frac = frac.reshape(ncols, ndepth, kcol)[:, 0]
    position = lax.dynamic_slice_in_dim(position, layer * share, share, axis=1).reshape(-1).astype(jnp.int32)
    frac = lax.dynamic_slice_in_dim(frac, layer * share, share, axis=1)

    def ordered(where):
        index = where // 2
        within = index % width_here
        row = ((index // width_here) * 2 + where % 2) * (width_here // lanes) + within // lanes
        return look_up(table, row, within % lanes).reshape(ncols, share)

    lower = ordered(position)
    shift = frac * (ordered(position + 1) - lower)
    roots = jnp.stack([lower, shift], axis=1)

    def near(full):
        full = full.reshape(ncols, ndepth, 2, width_here)
        full = lax.dynamic_index_in_dim(full, col, 0, keepdims=False)
        full = jnp.where(layer == 0, full, full[::-1])
        return jnp.transpose(full, (1, 0, 2)).reshape(2, ndepth * width_here)

    lines = jnp.stack([near(values), near(seams)], axis=2)

    if ncols == 4:
        total, norms = line_product(ncols, halves, roots, lines)
        return total / norms

    partner = lax.ppermute(halves, "depth", [(0, 1), (1, 0)])

    def step(chunk, dtype=jnp.bfloat16):
        mine = lax.dynamic_index_in_dim(roots, chunk, 0, keepdims=False)
        return [product(side, halves, partner, mine, lines, dtype) for side in range(2)]

    received = [[], []]
    for shift_by in range(1, ncols):
        parts = step((col + shift_by) % ncols)
        for side in range(2):
            moves = [(i, (i + shift_by) % ncols) for i in range(ncols)]
            received[side].append(lax.ppermute(parts[side], "col", moves))
    own = step(col, jnp.float32)
    last = own[1]

    mine = lax.dynamic_index_in_dim(roots, col, 0, keepdims=False)
    mine, _ = lax.optimization_barrier((mine, last))
    full_value = values.reshape(-1, 1)
    full_seam = seams.reshape(-1, 1)
    cauchy = full_seam / ((full_value - mine[0:1]) - mine[1:2])
    norms = jnp.sqrt(jnp.sum(cauchy * cauchy, axis=0, keepdims=True))

    out = combine(0, own[0], list(received[0]), norms, None)
    return combine(1, own[1], list(received[1]), norms, out)


def solution(mesh):
    in_specs = (P(None, "row", ("col", "depth")), P(None, ("col", "depth")), P("col"), P("col"))
    out_specs = P(None, "row", ("col", "depth"))
    return jax.shard_map(body, mesh=mesh, in_specs=in_specs, out_specs=out_specs, check_vma=False)
```

```python
import functools
import math

import jax
import jax.numpy as jnp
from jax import lax
from jax.experimental import pallas as pl
from jax.experimental.pallas import tpu as pltpu
from jax.sharding import PartitionSpec as P


def product_kernel(own_ref, par_ref, roots_ref, line_ref, out_ref, block_ref):
    inner = block_ref.shape[0]
    half = inner // 2
    step = math.gcd(inner, 64)

    @pl.when(pl.program_id(0) == 0)
    def _():
        lower = roots_ref[0:1, :]
        shift = roots_ref[1:2, :]

        def one(i, carry):
            rows = pl.ds(pl.multiple_of(i * step, step), step)
            value = line_ref[rows, 0:1]
            seam = line_ref[rows, 1:2]
            gap = (value - lower) - shift
            guess = pl.reciprocal(gap, approx=True)
            inverse = guess + guess * (1.0 - gap * guess)
            block_ref[rows, :] = (seam * inverse).astype(jnp.bfloat16)
            return carry

        lax.fori_loop(0, inner // step, one, 0)

    first = jnp.dot(own_ref[...], block_ref[0:half, :], preferred_element_type=jnp.float32)
    second = jnp.dot(par_ref[...], block_ref[half:inner, :], preferred_element_type=jnp.float32)
    out_ref[...] = (first + second).astype(out_ref.dtype)


def product(side, own, partner, roots, lines, dtype):
    rows = own.shape[1]
    half = own.shape[2]
    cols = roots.shape[1]
    tile = math.gcd(rows, 256)
    return pl.pallas_call(
        product_kernel,
        grid=(rows // tile,),
        in_specs=[
            pl.BlockSpec((None, tile, half), lambda i: (side, i, 0)),
            pl.BlockSpec((None, tile, half), lambda i: (side, i, 0)),
            pl.BlockSpec((2, cols), lambda i: (0, 0)),
            pl.BlockSpec((None, 2 * half, 2), lambda i: (side, 0, 0)),
        ],
        out_specs=pl.BlockSpec((tile, cols), lambda i: (i, 0)),
        out_shape=jax.ShapeDtypeStruct((rows, cols), dtype),
        scratch_shapes=[pltpu.VMEM((2 * half, cols), jnp.bfloat16)],
        cost_estimate=pl.CostEstimate(
            flops=4 * rows * half * cols,
            bytes_accessed=4 * rows * half + 4 * rows * cols,
            transcendentals=2 * half * cols,
        ),
        compiler_params=pltpu.CompilerParams(dimension_semantics=("arbitrary",)),
    )(own, partner, roots, lines)


def combine_kernel(count, *refs):
    own_ref = refs[0]
    norm_ref = refs[1 + count]
    out_ref = refs[-1]
    total = own_ref[...]
    for k in range(count):
        total = total + refs[1 + k][...].astype(jnp.float32)
    out_ref[...] = total / norm_ref[...]


def combine(side, own, parts, norms, whole):
    rows, cols = own.shape
    tile = math.gcd(rows, 256)
    count = len(parts)
    block = pl.BlockSpec((tile, cols), lambda i: (i, 0))
    operands = [own, *parts, norms]
    in_specs = [block] * (1 + count) + [pl.BlockSpec((1, cols), lambda i: (0, 0))]
    aliases = {}
    if whole is not None:
        aliases = {len(operands): 0}
        operands.append(whole)
        in_specs.append(pl.BlockSpec(memory_space=pl.ANY))
    return pl.pallas_call(
        functools.partial(combine_kernel, count),
        grid=(rows // tile,),
        in_specs=in_specs,
        out_specs=pl.BlockSpec((None, tile, cols), lambda i: (side, i, 0)),
        out_shape=jax.ShapeDtypeStruct((2, rows, cols), jnp.float32),
        input_output_aliases=aliases,
        cost_estimate=pl.CostEstimate(
            flops=(2 + count) * rows * cols, bytes_accessed=(8 + 2 * count) * rows * cols, transcendentals=0
        ),
        compiler_params=pltpu.CompilerParams(dimension_semantics=("arbitrary",)),
    )(*operands)


MESH = pl.DeviceIdType.MESH
LANES = 128
SLOTS = 10
SENDS = 3
LAG = 3
BLOCKS = 8


def line_kernel(n, nrow, halves, spectrum, wanted, fraction, out, norm, own, par, cauchy, total, got, send, square,
                squares, values, spots, shares, edge, seams, table, pieces, lines, roots, own_sem, par_send, par_got,
                send_sem, got_sem, square_send, square_got, value_send, value_got, spot_send, spot_got, share_send,
                share_got, edge_send, edge_got, free):
    c = lax.axis_index("col")
    d = lax.axis_index("depth")
    r = lax.axis_index("row")
    inner = cauchy.shape[1]
    half = inner // 2
    rows = own.shape[1]
    cols = cauchy.shape[2]
    tile = rows // BLOCKS
    chunks = 2 * BLOCKS
    groups = half // LANES
    shift_bits = half.bit_length() - 1
    place = 2 * c + d

    def part(b):
        return b // BLOCKS, pl.ds(pl.multiple_of((b % BLOCKS) * tile, tile), tile)

    def own_copy(b):
        side, where = part(b)
        return pltpu.make_async_copy(halves.at[side, where], own.at[side, where], own_sem.at[b])

    def send_to(source, target, sent, arrived, device):
        return pltpu.make_async_remote_copy(
            src_ref=source,
            dst_ref=target,
            send_sem=sent,
            recv_sem=arrived,
            device_id=device,
            device_id_type=MESH,
        )

    def par_copy(b):
        side, where = part(b)
        return send_to(
            halves.at[side, where], par.at[side, where], par_send.at[b], par_got.at[b], {"depth": 1 - d}
        )

    def square_copy(source, target):
        return send_to(
            square.at[target], squares.at[source], square_send.at[target], square_got.at[source], {"col": target}
        )

    def value_copy(k, source, target):
        return send_to(
            spectrum, values.at[source], value_send.at[k], value_got.at[source],
            {"col": target // 2, "depth": target % 2},
        )

    def spot_copy(k, source, target):
        return send_to(wanted, spots.at[source], spot_send.at[k], spot_got.at[source], {"col": target})

    def share_copy(k, source, target):
        return send_to(fraction, shares.at[source], share_send.at[k], share_got.at[source], {"col": target})

    def edge_copy(side, k, source, target):
        return send_to(
            edge.at[side], seams.at[source, side], edge_send.at[side, k], edge_got.at[source, side],
            {"row": target // 2, "depth": target % 2},
        )

    def each(count, act):
        def one(b, carry):
            act(b)
            return carry

        lax.fori_loop(0, count, one, 0)

    def edged(b):
        return (b == BLOCKS - 1) | (b == BLOCKS)

    own_copy(BLOCKS - 1).start()
    own_copy(BLOCKS).start()

    barrier = pltpu.get_barrier_semaphore()
    for k in range(1, 2 * n):
        other = (place + k) % (2 * n)
        pl.semaphore_signal(
            barrier, inc=1, device_id={"col": other // 2, "depth": other % 2}, device_id_type=MESH
        )
    for k in range(1, nrow):
        for depth in range(2):
            pl.semaphore_signal(
                barrier, inc=1, device_id={"row": (r + k) % nrow, "depth": depth}, device_id_type=MESH
            )

    @pl.loop(0, chunks)
    def _(b):
        @pl.when(jnp.logical_not(edged(b)))
        def _():
            own_copy(b).start()

    own_copy(BLOCKS - 1).wait()
    own_copy(BLOCKS).wait()
    for side in range(2):
        at = rows - 1 if side == 0 else 0
        base = at // 8 * 8

        @pl.when(r == (nrow - 1 if side == 0 else 0))
        def _():
            line = own[side, base : base + 8, :].astype(jnp.float32)[at - base : at - base + 1, :]
            for j in range(groups):
                edge[side, j : j + 1, :] = line[:, j * LANES : (j + 1) * LANES]

    pl.semaphore_wait(barrier, 2 * n - 1 + 2 * (nrow - 1))

    for k in range(1, 2 * n):
        value_copy(k, place, (place + k) % (2 * n)).start()
    for k in range(1, n):
        spot_copy(k, c, (c + k) % n).start()
        share_copy(k, c, (c + k) % n).start()
    for side in range(2):

        @pl.when(r == (nrow - 1 if side == 0 else 0))
        def _():
            for k in range(1, 2 * nrow):
                edge_copy(side, k, d, (2 * r + d + k) % (2 * nrow)).start()
            seams[d, side] = edge[side]

    each(chunks, lambda b: par_copy(b).start())
    values[place] = spectrum[...]
    spots[c] = wanted[...]
    shares[c] = fraction[...]

    for side in range(2):
        for near in range(2):
            source = d if near == 0 else 1 - d

            @pl.when((r != (nrow - 1 if side == 0 else 0)) | (near == 1))
            def _():
                edge_copy(side, 0, source, 2 * r + d).wait_recv()

    for k in range(1, 2 * n):
        other = (place + k) % (2 * n)
        value_copy(k, other, place).wait_recv()
    for k in range(1, n):
        other = (c + k) % n
        spot_copy(k, other, c).wait_recv()
        share_copy(k, other, c).wait_recv()

    @pl.loop(0, 2 * n)
    def _(g):
        full = values[g]
        for side in range(2):
            for j in range(groups):
                table[pl.ds((g * 2 + side) * groups + j, 1), :] = full[side : side + 1, j * LANES : (j + 1) * LANES]

    turned = []
    for near in range(2):
        source = d if near == 0 else 1 - d
        for side in range(2):
            at = pl.multiple_of(((2 * c + source) * 2 + side) * groups, groups)
            turned.append(table[pl.ds(at, groups), :])
            turned.append(seams[source, side])
    lines[...] = jnp.concatenate(turned, axis=0).T

    flipped = table[...].T
    high = flipped.astype(jnp.bfloat16)
    rest = flipped - high.astype(jnp.float32)
    middle = rest.astype(jnp.bfloat16)
    low = (rest - middle.astype(jnp.float32)).astype(jnp.bfloat16)
    pieces[0:LANES, :] = high
    pieces[LANES : 2 * LANES, :] = middle
    pieces[2 * LANES : 3 * LANES, :] = low

    def find_roots(way, target):
        tall = cols // LANES
        chosen = jnp.where(d == 0, spots[target, 0:tall, :], spots[target, tall : 2 * tall, :])
        weight = jnp.where(d == 0, shares[target, 0:tall, :], shares[target, tall : 2 * tall, :])
        hits, lanes = [], []
        entry = lax.broadcasted_iota(jnp.int32, (table.shape[0], LANES), 0)
        for above in range(2):
            for q in range(tall):
                where = chosen[q : q + 1, :] + above
                index = where >> 1
                within = index & (half - 1)
                row = ((index >> shift_bits) * 2 + (where & 1)) * groups + (within >> (LANES.bit_length() - 1))
                hits.append(jnp.where(entry == row, 1.0, 0.0).astype(jnp.bfloat16))
                lanes.append(within & (LANES - 1))
        hit = jnp.concatenate(hits, axis=1)
        lane = jnp.concatenate(lanes, axis=1)
        found = jnp.dot(pieces[...], hit, preferred_element_type=jnp.float32)
        found = (found[0:LANES] + found[LANES : 2 * LANES]) + found[2 * LANES : 3 * LANES]
        entry = lax.broadcasted_iota(jnp.int32, found.shape, 0)
        found = jnp.sum(jnp.where(entry == lane, found, 0.0), axis=0, keepdims=True)
        lower = found[:, 0:cols]
        weights = jnp.concatenate([weight[q : q + 1, :] for q in range(tall)], axis=1)
        roots[way, 0:1, :] = lower
        roots[way, 1:2, :] = weights * (found[:, cols : 2 * cols] - lower)

    def fill(way, side, target, forward):
        @pl.when(side == 0)
        def _():
            find_roots(way, target)

        lower = roots[way, 0:1, :]
        shift = roots[way, 1:2, :]

        def one(b, tally):
            near = b // groups
            turn = ((near * 2 + side) * 2) * groups + b % groups
            value = pltpu.roll(lines[...], LANES - turn, 1)[:, 0:1]
            seam = pltpu.roll(lines[...], LANES - groups - turn, 1)[:, 0:1]
            for m in range(LANES // 16):
                gap = (value[16 * m : 16 * m + 16] - lower) - shift
                guess = pl.reciprocal(gap, approx=True)
                inverse = guess + guess * (1.0 - gap * guess)
                terms = seam[16 * m : 16 * m + 16] * inverse
                at = pl.ds(pl.multiple_of(b * LANES + 16 * m, 16), 16)
                cauchy[way, at, :] = terms.astype(jnp.bfloat16)
                terms = terms * terms
                tally = tally + (terms[0:8] + terms[8:16])
            return tally

        tally = lax.fori_loop(0, inner // LANES, one, jnp.zeros(square.shape[1:], jnp.float32))

        @pl.when(side == 0)
        def _():
            square[target] = tally

        @pl.when(side == 1)
        def _():
            square[target] = square[target] + tally

        @pl.when((side == 1) & forward)
        def _():
            square_copy(c, target).start()

    def item(q, carry):
        s = q // 2
        way = q % 2
        far = c + way * (n - 1 - 2 * c)
        t = s - LAG * far
        u = t // chunks
        i = t - u * chunks
        side, where = part(i)
        mark = n - 1 - u
        target = mark + way * (n - 1 - 2 * mark)
        valid = (t >= 0) & (t < jnp.minimum(n - far, n - 1) * chunks)
        forward = valid & (mark > far)
        arrive = valid & (mark == far)
        first = arrive & (2 * far > n - 1)
        later = arrive & (2 * far <= n - 1)
        dot = forward | first
        incoming = valid & (far > 0)
        slot = t % SLOTS
        spot = t % SENDS

        def line_copy(at):
            return send_to(
                send.at[way, at % SENDS], got.at[way, at % SLOTS], send_sem.at[way, at % SENDS],
                got_sem.at[way, at % SLOTS], {"col": c + 1 - 2 * way},
            )

        @pl.when((way == 0) & (s < chunks))
        def _():
            @pl.when(jnp.logical_not(edged(s)))
            def _():
                own_copy(s).wait()

            par_copy(s).wait_recv()

        @pl.when(dot & (i % BLOCKS == 0))
        def _():
            fill(way, side, target, forward)

        @pl.when(dot)
        def _():
            a = jnp.dot(own[side, where, :], cauchy[way, 0:half, :], preferred_element_type=jnp.float32)
            b = jnp.dot(par[side, where, :], cauchy[way, half:inner, :], preferred_element_type=jnp.float32)
            total[...] = a + b

        @pl.when(incoming)
        def _():
            line_copy(t).wait_recv()

        @pl.when(forward & (t >= SENDS))
        def _():
            line_copy(t - SENDS).wait_send()

        @pl.when(forward & (far == 0))
        def _():
            send[way, spot] = total[...].astype(jnp.bfloat16)

        @pl.when(forward & (far > 0))
        def _():
            send[way, spot] = (total[...] + got[way, slot].astype(jnp.float32)).astype(jnp.bfloat16)

        @pl.when(first)
        def _():
            out[side, where, :] = total[...] + got[way, slot].astype(jnp.float32)

        @pl.when(later)
        def _():
            out[side, where, :] = out[side, where, :] + got[way, slot].astype(jnp.float32)

        @pl.when(incoming & (t + SLOTS < (n - far) * chunks))
        def _():
            pl.semaphore_signal(
                free.at[way], inc=1, device_id={"col": c - 1 + 2 * way}, device_id_type=MESH
            )

        @pl.when(forward)
        def _():
            @pl.when(t >= SLOTS)
            def _():
                pl.semaphore_wait(free.at[way], 1)

            line_copy(t).start()

        return carry

    steps = (n - 1) * (chunks + LAG)
    lax.fori_loop(0, 2 * steps, item, 0)

    for way in range(2):
        far = c + way * (n - 1 - 2 * c)

        @pl.when(far < n - 1)
        def _():
            for spot in range(SENDS):
                send_to(
                    send.at[way, spot], got.at[way, spot], send_sem.at[way, spot], got_sem.at[way, spot],
                    {"col": c + 1 - 2 * way},
                ).wait_send()

    each(chunks, lambda b: par_copy(b).wait_send())
    for k in range(1, 2 * n):
        value_copy(k, place, (place + k) % (2 * n)).wait_send()
    for side in range(2):

        @pl.when(r == (nrow - 1 if side == 0 else 0))
        def _():
            for k in range(1, 2 * nrow):
                edge_copy(side, k, d, (2 * r + d + k) % (2 * nrow)).wait_send()

    sums = square[c]
    for k in range(1, n):
        other = (c + k) % n
        spot_copy(k, c, other).wait_send()
        share_copy(k, c, other).wait_send()
        square_copy(c, other).wait_send()
        square_copy(other, c).wait_recv()
        sums = sums + squares[other]
    norm[...] = jnp.sqrt(jnp.sum(sums, axis=0, keepdims=True))


def line_product(n, nrow, halves, spectrum, wanted, fraction):
    _, rows, half = halves.shape
    kcol = wanted.shape[0]
    cols = kcol // 2
    tile = rows // BLOCKS
    chunks = 2 * BLOCKS
    groups = half // LANES
    dma = pltpu.SemaphoreType.DMA
    vmem = pl.BlockSpec(memory_space=pltpu.VMEM)
    return pl.pallas_call(
        functools.partial(line_kernel, n, nrow),
        in_specs=[pl.BlockSpec(memory_space=pl.ANY), vmem, vmem, vmem],
        out_specs=[vmem, vmem],
        out_shape=[
            pltpu.VMEM((2, rows, cols), jnp.float32),
            jax.ShapeDtypeStruct((1, cols), jnp.float32),
        ],
        scratch_shapes=[
            pltpu.VMEM((2, rows, half), jnp.bfloat16),
            pltpu.VMEM((2, rows, half), jnp.bfloat16),
            pltpu.VMEM((2, 2 * half, cols), jnp.bfloat16),
            pltpu.VMEM((tile, cols), jnp.float32),
            pltpu.VMEM((2, SLOTS, tile, cols), jnp.bfloat16),
            pltpu.VMEM((2, SENDS, tile, cols), jnp.bfloat16),
            pltpu.VMEM((n, 8, cols), jnp.float32),
            pltpu.VMEM((n, 8, cols), jnp.float32),
            pltpu.VMEM((2 * n, 2, half), jnp.float32),
            pltpu.VMEM((n, kcol // LANES, LANES), jnp.int32),
            pltpu.VMEM((n, kcol // LANES, LANES), jnp.float32),
            pltpu.VMEM((2, groups, LANES), jnp.float32),
            pltpu.VMEM((2, 2, groups, LANES), jnp.float32),
            pltpu.VMEM((4 * n * groups, LANES), jnp.float32),
            pltpu.VMEM((3 * LANES, 4 * n * groups), jnp.bfloat16),
            pltpu.VMEM((LANES, 8 * groups), jnp.float32),
            pltpu.VMEM((2, 2, cols), jnp.float32),
            dma((chunks,)),
            dma((chunks,)),
            dma((chunks,)),
            dma((2, SENDS)),
            dma((2, SLOTS)),
            dma((n,)),
            dma((n,)),
            dma((2 * n,)),
            dma((2 * n,)),
            dma((n,)),
            dma((n,)),
            dma((n,)),
            dma((n,)),
            dma((2, 2 * nrow)),
            dma((2, 2)),
            pltpu.SemaphoreType.REGULAR((2,)),
        ],
        cost_estimate=pl.CostEstimate(
            flops=8 * n * rows * half * cols,
            bytes_accessed=8 * rows * half + 8 * rows * cols,
            transcendentals=4 * n * half * cols,
        ),
        compiler_params=pltpu.CompilerParams(
            collective_id=0, has_side_effects=True, vmem_limit_bytes=55 * 1024 * 1024
        ),
    )(halves, spectrum, wanted.reshape(-1, LANES), fraction.reshape(-1, LANES))


def look_up(table, row, lane):
    pick = (row[:, None] == lax.broadcasted_iota(jnp.int32, (1, table.shape[0]), 1)).astype(jnp.float32)
    lines = jnp.dot(pick, table, precision=lax.Precision.HIGHEST, preferred_element_type=jnp.float32)
    lanes = lax.broadcasted_iota(jnp.int32, (1, table.shape[1]), 1)
    return jnp.sum(jnp.where(lane[:, None] == lanes, lines, 0.0), axis=1)


def body(halves, spectrum, wanted, fraction):
    ncols = lax.axis_size("col")
    ndepth = lax.axis_size("depth")
    nrow = lax.axis_size("row")
    col = lax.axis_index("col")
    layer = lax.axis_index("depth")
    rows_here = halves.shape[1]
    width_here = halves.shape[2]
    kcol = wanted.shape[0]
    share = kcol // ndepth

    if ncols == 4 and 8 * width_here == LANES * LANES:
        total, norms = line_product(ncols, nrow, halves, spectrum, wanted, fraction)
        return total / norms

    edges = jnp.stack([halves[0, rows_here - 1], halves[1, 0]])
    edges = lax.all_gather(edges, "row", axis=0, tiled=False)
    seam = jnp.stack([edges[nrow - 1, 0], edges[0, 1]]).astype(jnp.float32)

    lanes = math.gcd(width_here, 128)
    flat = jnp.concatenate(
        [spectrum.reshape(-1), seam.reshape(-1), wanted.astype(jnp.float32), fraction]
    )
    flat = lax.all_gather(flat, ("col", "depth"), axis=0, tiled=False)
    pieces = jnp.split(flat, [2 * width_here, 4 * width_here, 4 * width_here + kcol], axis=1)
    values, seams, position, frac = pieces
    table = values.reshape(-1, lanes)
    position = position.reshape(ncols, ndepth, kcol)[:, 0]
    frac = frac.reshape(ncols, ndepth, kcol)[:, 0]
    position = lax.dynamic_slice_in_dim(position, layer * share, share, axis=1).reshape(-1).astype(jnp.int32)
    frac = lax.dynamic_slice_in_dim(frac, layer * share, share, axis=1)

    def ordered(where):
        index = where // 2
        within = index % width_here
        row = ((index // width_here) * 2 + where % 2) * (width_here // lanes) + within // lanes
        return look_up(table, row, within % lanes).reshape(ncols, share)

    lower = ordered(position)
    shift = frac * (ordered(position + 1) - lower)
    roots = jnp.stack([lower, shift], axis=1)

    def near(full):
        full = full.reshape(ncols, ndepth, 2, width_here)
        full = lax.dynamic_index_in_dim(full, col, 0, keepdims=False)
        full = jnp.where(layer == 0, full, full[::-1])
        return jnp.transpose(full, (1, 0, 2)).reshape(2, ndepth * width_here)

    lines = jnp.stack([near(values), near(seams)], axis=2)

    partner = lax.ppermute(halves, "depth", [(0, 1), (1, 0)])

    def step(chunk, dtype=jnp.bfloat16):
        mine = lax.dynamic_index_in_dim(roots, chunk, 0, keepdims=False)
        return [product(side, halves, partner, mine, lines, dtype) for side in range(2)]

    received = [[], []]
    for shift_by in range(1, ncols):
        parts = step((col + shift_by) % ncols)
        for side in range(2):
            moves = [(i, (i + shift_by) % ncols) for i in range(ncols)]
            received[side].append(lax.ppermute(parts[side], "col", moves))
    own = step(col, jnp.float32)
    last = own[1]

    mine = lax.dynamic_index_in_dim(roots, col, 0, keepdims=False)
    mine, _ = lax.optimization_barrier((mine, last))
    full_value = values.reshape(-1, 1)
    full_seam = seams.reshape(-1, 1)
    cauchy = full_seam / ((full_value - mine[0:1]) - mine[1:2])
    norms = jnp.sqrt(jnp.sum(cauchy * cauchy, axis=0, keepdims=True))

    out = combine(0, own[0], list(received[0]), norms, None)
    return combine(1, own[1], list(received[1]), norms, out)


def solution(mesh):
    in_specs = (P(None, "row", ("col", "depth")), P(None, ("col", "depth")), P("col"), P("col"))
    out_specs = P(None, "row", ("col", "depth"))
    return jax.shard_map(body, mesh=mesh, in_specs=in_specs, out_specs=out_specs, check_vma=False)
```

```python
import functools
import math

import jax
import jax.numpy as jnp
from jax import lax
from jax.experimental import pallas as pl
from jax.experimental.pallas import tpu as pltpu
from jax.sharding import PartitionSpec as P


def product_kernel(own_ref, par_ref, roots_ref, line_ref, out_ref, block_ref):
    inner = block_ref.shape[0]
    half = inner // 2
    step = math.gcd(inner, 64)

    @pl.when(pl.program_id(0) == 0)
    def _():
        lower = roots_ref[0:1, :]
        shift = roots_ref[1:2, :]

        def one(i, carry):
            rows = pl.ds(pl.multiple_of(i * step, step), step)
            value = line_ref[rows, 0:1]
            seam = line_ref[rows, 1:2]
            gap = (value - lower) - shift
            guess = pl.reciprocal(gap, approx=True)
            inverse = guess + guess * (1.0 - gap * guess)
            block_ref[rows, :] = (seam * inverse).astype(jnp.bfloat16)
            return carry

        lax.fori_loop(0, inner // step, one, 0)

    first = jnp.dot(own_ref[...], block_ref[0:half, :], preferred_element_type=jnp.float32)
    second = jnp.dot(par_ref[...], block_ref[half:inner, :], preferred_element_type=jnp.float32)
    out_ref[...] = (first + second).astype(out_ref.dtype)


def product(side, own, partner, roots, lines, dtype):
    rows = own.shape[1]
    half = own.shape[2]
    cols = roots.shape[1]
    tile = math.gcd(rows, 256)
    return pl.pallas_call(
        product_kernel,
        grid=(rows // tile,),
        in_specs=[
            pl.BlockSpec((None, tile, half), lambda i: (side, i, 0)),
            pl.BlockSpec((None, tile, half), lambda i: (side, i, 0)),
            pl.BlockSpec((2, cols), lambda i: (0, 0)),
            pl.BlockSpec((None, 2 * half, 2), lambda i: (side, 0, 0)),
        ],
        out_specs=pl.BlockSpec((tile, cols), lambda i: (i, 0)),
        out_shape=jax.ShapeDtypeStruct((rows, cols), dtype),
        scratch_shapes=[pltpu.VMEM((2 * half, cols), jnp.bfloat16)],
        cost_estimate=pl.CostEstimate(
            flops=4 * rows * half * cols,
            bytes_accessed=4 * rows * half + 4 * rows * cols,
            transcendentals=2 * half * cols,
        ),
        compiler_params=pltpu.CompilerParams(dimension_semantics=("arbitrary",)),
    )(own, partner, roots, lines)


def combine_kernel(count, *refs):
    own_ref = refs[0]
    norm_ref = refs[1 + count]
    out_ref = refs[-1]
    total = own_ref[...]
    for k in range(count):
        total = total + refs[1 + k][...].astype(jnp.float32)
    out_ref[...] = total / norm_ref[...]


def combine(side, own, parts, norms, whole):
    rows, cols = own.shape
    tile = math.gcd(rows, 256)
    count = len(parts)
    block = pl.BlockSpec((tile, cols), lambda i: (i, 0))
    operands = [own, *parts, norms]
    in_specs = [block] * (1 + count) + [pl.BlockSpec((1, cols), lambda i: (0, 0))]
    aliases = {}
    if whole is not None:
        aliases = {len(operands): 0}
        operands.append(whole)
        in_specs.append(pl.BlockSpec(memory_space=pl.ANY))
    return pl.pallas_call(
        functools.partial(combine_kernel, count),
        grid=(rows // tile,),
        in_specs=in_specs,
        out_specs=pl.BlockSpec((None, tile, cols), lambda i: (side, i, 0)),
        out_shape=jax.ShapeDtypeStruct((2, rows, cols), jnp.float32),
        input_output_aliases=aliases,
        cost_estimate=pl.CostEstimate(
            flops=(2 + count) * rows * cols, bytes_accessed=(8 + 2 * count) * rows * cols, transcendentals=0
        ),
        compiler_params=pltpu.CompilerParams(dimension_semantics=("arbitrary",)),
    )(*operands)


MESH = pl.DeviceIdType.MESH
LANES = 128
SLOTS = 10
SENDS = 3
LAG = 3
BLOCKS = 4
SPLIT = 2
STEP = 64


def line_kernel(n, nrow, halves, spectrum, wanted, fraction, out, norm, own, par, cauchy, total, got, send, square,
                squares, values, spots, shares, ends, edge, seams, table, pieces, lines, wide, roots, own_sem, end_sem,
                par_send, par_got, send_sem, got_sem, square_send, square_got, value_send, value_got, spot_send,
                spot_got, share_send, share_got, edge_send, edge_got, free):
    c = lax.axis_index("col")
    d = lax.axis_index("depth")
    r = lax.axis_index("row")
    inner = cauchy.shape[1]
    half = inner // 2
    rows = own.shape[1]
    cols = cauchy.shape[2]
    tile = rows // BLOCKS
    blocks = 2 * BLOCKS
    chunks = blocks * SPLIT
    groups = half // LANES
    shift_bits = half.bit_length() - 1
    place = 2 * c + d

    def part(b):
        return b // BLOCKS, pl.ds(pl.multiple_of((b % BLOCKS) * tile, tile), tile)

    def own_copy(b):
        side, where = part(b)
        return pltpu.make_async_copy(halves.at[side, where], own.at[side, where], own_sem.at[b])

    def send_to(source, target, sent, arrived, device):
        return pltpu.make_async_remote_copy(
            src_ref=source,
            dst_ref=target,
            send_sem=sent,
            recv_sem=arrived,
            device_id=device,
            device_id_type=MESH,
        )

    def par_copy(b):
        side, where = part(b)
        return send_to(
            halves.at[side, where], par.at[side, where], par_send.at[b], par_got.at[b], {"depth": 1 - d}
        )

    def square_copy(source, target):
        return send_to(
            square.at[target], squares.at[source], square_send.at[target], square_got.at[source], {"col": target}
        )

    def value_copy(source, target):
        return send_to(
            spectrum, values.at[source], value_send.at[target], value_got.at[source],
            {"col": target // 2, "depth": target % 2},
        )

    def spot_copy(source, target):
        return send_to(wanted, spots.at[source], spot_send.at[target], spot_got.at[source], {"col": target})

    def share_copy(source, target):
        return send_to(fraction, shares.at[source], share_send.at[target], share_got.at[source], {"col": target})

    def end_copy(side):
        at = (rows - 1 if side == 0 else 0) // 8 * 8
        return pltpu.make_async_copy(halves.at[side, pl.ds(at, 8)], ends.at[side], end_sem.at[side])

    step = math.gcd(inner, STEP)

    def edge_copy(side, k, source, target):
        return send_to(
            edge.at[side], seams.at[source, side], edge_send.at[side, k], edge_got.at[source, side],
            {"row": target // 2, "depth": target % 2},
        )

    def each(count, act):
        def one(b, carry):
            act(b)
            return carry

        lax.fori_loop(0, count, one, 0)

    for side in range(2):
        end_copy(side).start()

    barrier = pltpu.get_barrier_semaphore()
    for k in range(1, 2 * n):
        other = (place + k) % (2 * n)
        pl.semaphore_signal(
            barrier, inc=1, device_id={"col": other // 2, "depth": other % 2}, device_id_type=MESH
        )
    for k in range(1, nrow):
        for depth in range(2):
            pl.semaphore_signal(
                barrier, inc=1, device_id={"row": (r + k) % nrow, "depth": depth}, device_id_type=MESH
            )

    each(blocks, lambda b: own_copy(b).start())
    for side in range(2):
        end_copy(side).wait()
        at = (rows - 1 if side == 0 else 0) % 8

        @pl.when(r == (nrow - 1 if side == 0 else 0))
        def _():
            line = ends[side].astype(jnp.float32)[at : at + 1, :]
            for j in range(groups):
                edge[side, j : j + 1, :] = line[:, j * LANES : (j + 1) * LANES]

    pl.semaphore_wait(barrier, 2 * n - 1 + 2 * (nrow - 1))

    for gone in range(n - 1, 0, -1):
        for other in (c + gone, c - gone):

            @pl.when((other >= 0) & (other < n))
            def _():
                spot_copy(c, other).start()
                share_copy(c, other).start()
                for depth in range(2):
                    value_copy(place, 2 * other + depth).start()

    value_copy(place, 2 * c + 1 - d).start()
    for side in range(2):

        @pl.when(r == (nrow - 1 if side == 0 else 0))
        def _():
            for k in range(1, 2 * nrow):
                edge_copy(side, k, d, (2 * r + d + k) % (2 * nrow)).start()
            seams[d, side] = edge[side]

    each(blocks, lambda b: par_copy(b).start())
    values[place] = spectrum[...]
    spots[c] = wanted[...]
    shares[c] = fraction[...]

    for side in range(2):
        for near in range(2):
            source = d if near == 0 else 1 - d

            @pl.when((r != (nrow - 1 if side == 0 else 0)) | (near == 1))
            def _():
                edge_copy(side, 0, source, 2 * r + d).wait_recv()

    for k in range(1, 2 * n):
        other = (place + k) % (2 * n)
        value_copy(other, place).wait_recv()
    for k in range(1, n):
        other = (c + k) % n
        spot_copy(other, c).wait_recv()
        share_copy(other, c).wait_recv()

    @pl.loop(0, 2 * n)
    def _(g):
        full = values[g]
        for side in range(2):
            for j in range(groups):
                table[pl.ds((g * 2 + side) * groups + j, 1), :] = full[side : side + 1, j * LANES : (j + 1) * LANES]

    for side in range(2):
        turned = []
        for near in range(2):
            source = d if near == 0 else 1 - d
            at = pl.multiple_of(((2 * c + source) * 2 + side) * groups, groups)
            turned.append(table[pl.ds(at, groups), :])
            turned.append(seams[source, side])
        lines[side] = jnp.concatenate(turned, axis=0).T

    flipped = table[...].T
    high = flipped.astype(jnp.bfloat16)
    rest = flipped - high.astype(jnp.float32)
    middle = rest.astype(jnp.bfloat16)
    low = (rest - middle.astype(jnp.float32)).astype(jnp.bfloat16)
    pieces[0:LANES, :] = high
    pieces[LANES : 2 * LANES, :] = middle
    pieces[2 * LANES : 3 * LANES, :] = low

    def widen(side):
        full = lines[side]
        for near in range(2):
            for kind in range(2):
                for j in range(groups):
                    column = (near * 2 + kind) * groups + j
                    at = (near * groups + j) * LANES
                    wide[kind, side, at : at + LANES, :] = jnp.broadcast_to(
                        full[:, column : column + 1], (LANES, LANES)
                    )

    def find_roots(way, target, piece):
        tall = cols // LANES
        begin = d * SPLIT + piece

        def choose(ref):
            full = ref[target]
            choice = full[0:tall, :]
            for k in range(1, 2 * SPLIT):
                choice = jnp.where(begin == k, full[k * tall : (k + 1) * tall, :], choice)
            return choice

        chosen = choose(spots)
        weight = choose(shares)
        hits, lanes = [], []
        entry = lax.broadcasted_iota(jnp.int32, (table.shape[0], LANES), 0)
        for above in range(2):
            for q in range(tall):
                where = chosen[q : q + 1, :] + above
                index = where >> 1
                within = index & (half - 1)
                row = ((index >> shift_bits) * 2 + (where & 1)) * groups + (within >> (LANES.bit_length() - 1))
                hits.append(jnp.where(entry == row, 1.0, 0.0).astype(jnp.bfloat16))
                lanes.append(within & (LANES - 1))
        hit = jnp.concatenate(hits, axis=1)
        lane = jnp.concatenate(lanes, axis=1)
        found = jnp.dot(pieces[...], hit, preferred_element_type=jnp.float32)
        found = (found[0:LANES] + found[LANES : 2 * LANES]) + found[2 * LANES : 3 * LANES]
        entry = lax.broadcasted_iota(jnp.int32, found.shape, 0)
        found = jnp.sum(jnp.where(entry == lane, found, 0.0), axis=0, keepdims=True)
        lower = found[:, 0:cols]
        weights = jnp.concatenate([weight[q : q + 1, :] for q in range(tall)], axis=1)
        roots[way, piece, 0:1, :] = lower
        roots[way, piece, 1:2, :] = weights * (found[:, cols : 2 * cols] - lower)

    def fill(way, side, piece, target, forward):
        @pl.when(side == 0)
        def _():
            find_roots(way, target, piece)

        def one(b, tallies):
            at = pl.ds(pl.multiple_of(b * step, step), step)
            value = wide[0, side, at, :]
            seam = wide[1, side, at, :]
            sums = []
            for q in range(cols // LANES):
                lanes = slice(q * LANES, (q + 1) * LANES)
                gap = (value - roots[way, piece, 0:1, lanes]) - roots[way, piece, 1:2, lanes]
                guess = pl.reciprocal(gap, approx=True)
                terms = (seam * guess) * (2.0 - gap * guess)
                cauchy[way, at, lanes] = terms.astype(jnp.bfloat16)
                terms = terms * terms
                tally = tallies[q]
                for j in range(step // 8):
                    tally = tally + terms[8 * j : 8 * j + 8, :]
                sums.append(tally)
            return tuple(sums)

        zero = jnp.zeros((8, LANES), jnp.float32)
        tallies = lax.fori_loop(0, inner // step, one, (zero,) * (cols // LANES))
        tally = jnp.concatenate(tallies, axis=1)

        @pl.when(side == 0)
        def _():
            square[target, piece] = tally

        @pl.when(side == 1)
        def _():
            square[target, piece] = square[target, piece] + tally

        @pl.when((side == 1) & (piece == SPLIT - 1) & forward)
        def _():
            square_copy(c, target).start()

    def item(q, carry):
        s = q // 2
        way = q % 2
        far = c + way * (n - 1 - 2 * c)
        t = s - LAG * far
        u = t // chunks
        i = t - u * chunks
        side = i // (BLOCKS * SPLIT)
        piece = (i // BLOCKS) % SPLIT
        where = pl.ds(pl.multiple_of((i % BLOCKS) * tile, tile), tile)
        held = pl.ds(pl.multiple_of(piece * cols, cols), cols)
        mark = n - 1 - u
        target = mark + way * (n - 1 - 2 * mark)
        valid = (t >= 0) & (t < jnp.minimum(n - far, n - 1) * chunks)
        forward = valid & (mark > far)
        arrive = valid & (mark == far)
        first = arrive & (2 * far > n - 1)
        later = arrive & (2 * far <= n - 1)
        dot = forward | first
        incoming = valid & (far > 0)
        slot = t % SLOTS
        spot = t % SENDS

        def line_copy(at):
            return send_to(
                send.at[way, at % SENDS], got.at[way, at % SLOTS], send_sem.at[way, at % SENDS],
                got_sem.at[way, at % SLOTS], {"col": c + 1 - 2 * way},
            )

        @pl.when((way == 0) & (s < 2))
        def _():
            widen(s)

        @pl.when((way == 0) & (s < chunks) & (s % (BLOCKS * SPLIT) < BLOCKS))
        def _():
            b = s // (BLOCKS * SPLIT) * BLOCKS + s % BLOCKS
            own_copy(b).wait()
            par_copy(b).wait_recv()

        @pl.when(dot & (i % BLOCKS == 0))
        def _():
            fill(way, side, piece, target, forward)

        @pl.when(dot)
        def _():
            a = jnp.dot(own[side, where, :], cauchy[way, 0:half, :], preferred_element_type=jnp.float32)
            b = jnp.dot(par[side, where, :], cauchy[way, half:inner, :], preferred_element_type=jnp.float32)
            total[...] = a + b

        @pl.when(incoming)
        def _():
            line_copy(t).wait_recv()

        @pl.when(forward & (t >= SENDS))
        def _():
            line_copy(t - SENDS).wait_send()

        @pl.when(forward & (far == 0))
        def _():
            send[way, spot] = total[...].astype(jnp.bfloat16)

        @pl.when(forward & (far > 0))
        def _():
            send[way, spot] = (total[...] + got[way, slot].astype(jnp.float32)).astype(jnp.bfloat16)

        @pl.when(first)
        def _():
            out[side, where, held] = total[...] + got[way, slot].astype(jnp.float32)

        @pl.when(later)
        def _():
            out[side, where, held] = out[side, where, held] + got[way, slot].astype(jnp.float32)

        @pl.when(incoming & (t + SLOTS < (n - far) * chunks))
        def _():
            pl.semaphore_signal(
                free.at[way], inc=1, device_id={"col": c - 1 + 2 * way}, device_id_type=MESH
            )

        @pl.when(forward)
        def _():
            @pl.when(t >= SLOTS)
            def _():
                pl.semaphore_wait(free.at[way], 1)

            line_copy(t).start()

        return carry

    steps = (n - 1) * chunks + LAG
    lax.fori_loop(0, 2 * steps, item, 0)

    for way in range(2):
        far = c + way * (n - 1 - 2 * c)

        @pl.when(far < n - 1)
        def _():
            for spot in range(SENDS):
                send_to(
                    send.at[way, spot], got.at[way, spot], send_sem.at[way, spot], got_sem.at[way, spot],
                    {"col": c + 1 - 2 * way},
                ).wait_send()

    each(blocks, lambda b: par_copy(b).wait_send())
    for k in range(1, 2 * n):
        value_copy(place, (place + k) % (2 * n)).wait_send()
    for side in range(2):

        @pl.when(r == (nrow - 1 if side == 0 else 0))
        def _():
            for k in range(1, 2 * nrow):
                edge_copy(side, k, d, (2 * r + d + k) % (2 * nrow)).wait_send()

    sums = square[c]
    for k in range(1, n):
        other = (c + k) % n
        spot_copy(c, other).wait_send()
        share_copy(c, other).wait_send()
        square_copy(c, other).wait_send()
        square_copy(other, c).wait_recv()
        sums = sums + squares[other]
    for piece in range(SPLIT):
        total_square = jnp.sum(sums[piece], axis=0, keepdims=True)
        norm[:, piece * cols : (piece + 1) * cols] = jnp.sqrt(total_square)


def divide_kernel(total, norm, out, ready, sem):
    rows = ready.shape[1]
    per_side = total.shape[1] // rows
    count = 2 * per_side

    def put(k):
        where = pl.ds(pl.multiple_of((k % per_side) * rows, rows), rows)
        return pltpu.make_async_copy(ready.at[k % 4], out.at[k // per_side, where], sem.at[k % 4])

    @pl.loop(0, count)
    def _(k):
        @pl.when(k >= 4)
        def _():
            put(k - 4).wait()

        where = pl.ds(pl.multiple_of((k % per_side) * rows, rows), rows)
        ready[k % 4] = total[k // per_side, where, :] / norm[...]
        put(k).start()

    for k in range(count - 4, count):
        put(k).wait()


def divide(total, norm):
    _, rows, cols = total.shape
    tile = rows // 8
    vmem = pl.BlockSpec(memory_space=pltpu.VMEM)
    return pl.pallas_call(
        divide_kernel,
        in_specs=[vmem, vmem],
        out_specs=pl.BlockSpec(memory_space=pl.ANY),
        out_shape=jax.ShapeDtypeStruct(total.shape, jnp.float32),
        scratch_shapes=[pltpu.VMEM((4, tile, cols), jnp.float32), pltpu.SemaphoreType.DMA((4,))],
        cost_estimate=pl.CostEstimate(
            flops=2 * rows * cols, bytes_accessed=16 * rows * cols, transcendentals=2 * rows * cols
        ),
        compiler_params=pltpu.CompilerParams(vmem_limit_bytes=16 * 1024 * 1024),
    )(total, norm)


def line_product(n, nrow, halves, spectrum, wanted, fraction):
    _, rows, half = halves.shape
    kcol = wanted.shape[0]
    share = kcol // 2
    cols = share // SPLIT
    tile = rows // BLOCKS
    blocks = 2 * BLOCKS
    groups = half // LANES
    dma = pltpu.SemaphoreType.DMA
    vmem = pl.BlockSpec(memory_space=pltpu.VMEM)
    return pl.pallas_call(
        functools.partial(line_kernel, n, nrow),
        in_specs=[pl.BlockSpec(memory_space=pl.ANY), vmem, vmem, vmem],
        out_specs=[vmem, vmem],
        out_shape=[
            pltpu.VMEM((2, rows, share), jnp.float32),
            pltpu.VMEM((1, share), jnp.float32),
        ],
        scratch_shapes=[
            pltpu.VMEM((2, rows, half), jnp.bfloat16),
            pltpu.VMEM((2, rows, half), jnp.bfloat16),
            pltpu.VMEM((2, 2 * half, cols), jnp.bfloat16),
            pltpu.VMEM((tile, cols), jnp.float32),
            pltpu.VMEM((2, SLOTS, tile, cols), jnp.bfloat16),
            pltpu.VMEM((2, SENDS, tile, cols), jnp.bfloat16),
            pltpu.VMEM((n, SPLIT, 8, cols), jnp.float32),
            pltpu.VMEM((n, SPLIT, 8, cols), jnp.float32),
            pltpu.VMEM((2 * n, 2, half), jnp.float32),
            pltpu.VMEM((n, kcol // LANES, LANES), jnp.int32),
            pltpu.VMEM((n, kcol // LANES, LANES), jnp.float32),
            pltpu.VMEM((2, 8, half), jnp.bfloat16),
            pltpu.VMEM((2, groups, LANES), jnp.float32),
            pltpu.VMEM((2, 2, groups, LANES), jnp.float32),
            pltpu.VMEM((4 * n * groups, LANES), jnp.float32),
            pltpu.VMEM((3 * LANES, 4 * n * groups), jnp.bfloat16),
            pltpu.VMEM((2, LANES, 4 * groups), jnp.float32),
            pltpu.VMEM((2, 2, 2 * half, LANES), jnp.float32),
            pltpu.VMEM((2, SPLIT, 2, cols), jnp.float32),
            dma((blocks,)),
            dma((2,)),
            dma((blocks,)),
            dma((blocks,)),
            dma((2, SENDS)),
            dma((2, SLOTS)),
            dma((n,)),
            dma((n,)),
            dma((2 * n,)),
            dma((2 * n,)),
            dma((n,)),
            dma((n,)),
            dma((n,)),
            dma((n,)),
            dma((2, 2 * nrow)),
            dma((2, 2)),
            pltpu.SemaphoreType.REGULAR((2,)),
        ],
        cost_estimate=pl.CostEstimate(
            flops=8 * n * rows * half * share,
            bytes_accessed=8 * rows * half + 8 * rows * share,
            transcendentals=4 * n * half * share,
        ),
        compiler_params=pltpu.CompilerParams(
            collective_id=0, has_side_effects=True, vmem_limit_bytes=55 * 1024 * 1024
        ),
    )(halves, spectrum, wanted.reshape(-1, LANES), fraction.reshape(-1, LANES))


def look_up(table, row, lane):
    pick = (row[:, None] == lax.broadcasted_iota(jnp.int32, (1, table.shape[0]), 1)).astype(jnp.float32)
    lines = jnp.dot(pick, table, precision=lax.Precision.HIGHEST, preferred_element_type=jnp.float32)
    lanes = lax.broadcasted_iota(jnp.int32, (1, table.shape[1]), 1)
    return jnp.sum(jnp.where(lane[:, None] == lanes, lines, 0.0), axis=1)


def body(halves, spectrum, wanted, fraction):
    ncols = lax.axis_size("col")
    ndepth = lax.axis_size("depth")
    nrow = lax.axis_size("row")
    col = lax.axis_index("col")
    layer = lax.axis_index("depth")
    rows_here = halves.shape[1]
    width_here = halves.shape[2]
    kcol = wanted.shape[0]
    share = kcol // ndepth

    if ncols == 4 and 8 * width_here == LANES * LANES:
        total, norms = line_product(ncols, nrow, halves, spectrum, wanted, fraction)
        return divide(total, norms)

    edges = jnp.stack([halves[0, rows_here - 1], halves[1, 0]])
    edges = lax.all_gather(edges, "row", axis=0, tiled=False)
    seam = jnp.stack([edges[nrow - 1, 0], edges[0, 1]]).astype(jnp.float32)

    lanes = math.gcd(width_here, 128)
    flat = jnp.concatenate(
        [spectrum.reshape(-1), seam.reshape(-1), wanted.astype(jnp.float32), fraction]
    )
    flat = lax.all_gather(flat, ("col", "depth"), axis=0, tiled=False)
    pieces = jnp.split(flat, [2 * width_here, 4 * width_here, 4 * width_here + kcol], axis=1)
    values, seams, position, frac = pieces
    table = values.reshape(-1, lanes)
    position = position.reshape(ncols, ndepth, kcol)[:, 0]
    frac = frac.reshape(ncols, ndepth, kcol)[:, 0]
    position = lax.dynamic_slice_in_dim(position, layer * share, share, axis=1).reshape(-1).astype(jnp.int32)
    frac = lax.dynamic_slice_in_dim(frac, layer * share, share, axis=1)

    def ordered(where):
        index = where // 2
        within = index % width_here
        row = ((index // width_here) * 2 + where % 2) * (width_here // lanes) + within // lanes
        return look_up(table, row, within % lanes).reshape(ncols, share)

    lower = ordered(position)
    shift = frac * (ordered(position + 1) - lower)
    roots = jnp.stack([lower, shift], axis=1)

    def near(full):
        full = full.reshape(ncols, ndepth, 2, width_here)
        full = lax.dynamic_index_in_dim(full, col, 0, keepdims=False)
        full = jnp.where(layer == 0, full, full[::-1])
        return jnp.transpose(full, (1, 0, 2)).reshape(2, ndepth * width_here)

    lines = jnp.stack([near(values), near(seams)], axis=2)

    partner = lax.ppermute(halves, "depth", [(0, 1), (1, 0)])

    def step(chunk, dtype=jnp.bfloat16):
        mine = lax.dynamic_index_in_dim(roots, chunk, 0, keepdims=False)
        return [product(side, halves, partner, mine, lines, dtype) for side in range(2)]

    received = [[], []]
    for shift_by in range(1, ncols):
        parts = step((col + shift_by) % ncols)
        for side in range(2):
            moves = [(i, (i + shift_by) % ncols) for i in range(ncols)]
            received[side].append(lax.ppermute(parts[side], "col", moves))
    own = step(col, jnp.float32)
    last = own[1]

    mine = lax.dynamic_index_in_dim(roots, col, 0, keepdims=False)
    mine, _ = lax.optimization_barrier((mine, last))
    full_value = values.reshape(-1, 1)
    full_seam = seams.reshape(-1, 1)
    cauchy = full_seam / ((full_value - mine[0:1]) - mine[1:2])
    norms = jnp.sqrt(jnp.sum(cauchy * cauchy, axis=0, keepdims=True))

    out = combine(0, own[0], list(received[0]), norms, None)
    return combine(1, own[1], list(received[1]), norms, out)


def solution(mesh):
    in_specs = (P(None, "row", ("col", "depth")), P(None, ("col", "depth")), P("col"), P("col"))
    out_specs = P(None, "row", ("col", "depth"))
    return jax.shard_map(body, mesh=mesh, in_specs=in_specs, out_specs=out_specs, check_vma=False)
```

```python
import functools
import math

import jax
import jax.numpy as jnp
from jax import lax
from jax.experimental import pallas as pl
from jax.experimental.pallas import tpu as pltpu
from jax.sharding import PartitionSpec as P


def product_kernel(own_ref, par_ref, roots_ref, line_ref, out_ref, block_ref):
    inner = block_ref.shape[0]
    half = inner // 2
    step = math.gcd(inner, 64)

    @pl.when(pl.program_id(0) == 0)
    def _():
        lower = roots_ref[0:1, :]
        shift = roots_ref[1:2, :]

        def one(i, carry):
            rows = pl.ds(pl.multiple_of(i * step, step), step)
            value = line_ref[rows, 0:1]
            seam = line_ref[rows, 1:2]
            gap = (value - lower) - shift
            guess = pl.reciprocal(gap, approx=True)
            inverse = guess + guess * (1.0 - gap * guess)
            block_ref[rows, :] = (seam * inverse).astype(jnp.bfloat16)
            return carry

        lax.fori_loop(0, inner // step, one, 0)

    first = jnp.dot(own_ref[...], block_ref[0:half, :], preferred_element_type=jnp.float32)
    second = jnp.dot(par_ref[...], block_ref[half:inner, :], preferred_element_type=jnp.float32)
    out_ref[...] = (first + second).astype(out_ref.dtype)


def product(side, own, partner, roots, lines, dtype):
    rows = own.shape[1]
    half = own.shape[2]
    cols = roots.shape[1]
    tile = math.gcd(rows, 256)
    return pl.pallas_call(
        product_kernel,
        grid=(rows // tile,),
        in_specs=[
            pl.BlockSpec((None, tile, half), lambda i: (side, i, 0)),
            pl.BlockSpec((None, tile, half), lambda i: (side, i, 0)),
            pl.BlockSpec((2, cols), lambda i: (0, 0)),
            pl.BlockSpec((None, 2 * half, 2), lambda i: (side, 0, 0)),
        ],
        out_specs=pl.BlockSpec((tile, cols), lambda i: (i, 0)),
        out_shape=jax.ShapeDtypeStruct((rows, cols), dtype),
        scratch_shapes=[pltpu.VMEM((2 * half, cols), jnp.bfloat16)],
        cost_estimate=pl.CostEstimate(
            flops=4 * rows * half * cols,
            bytes_accessed=4 * rows * half + 4 * rows * cols,
            transcendentals=2 * half * cols,
        ),
        compiler_params=pltpu.CompilerParams(dimension_semantics=("arbitrary",)),
    )(own, partner, roots, lines)


def combine_kernel(count, *refs):
    own_ref = refs[0]
    norm_ref = refs[1 + count]
    out_ref = refs[-1]
    total = own_ref[...]
    for k in range(count):
        total = total + refs[1 + k][...].astype(jnp.float32)
    out_ref[...] = total / norm_ref[...]


def combine(side, own, parts, norms, whole):
    rows, cols = own.shape
    tile = math.gcd(rows, 256)
    count = len(parts)
    block = pl.BlockSpec((tile, cols), lambda i: (i, 0))
    operands = [own, *parts, norms]
    in_specs = [block] * (1 + count) + [pl.BlockSpec((1, cols), lambda i: (0, 0))]
    aliases = {}
    if whole is not None:
        aliases = {len(operands): 0}
        operands.append(whole)
        in_specs.append(pl.BlockSpec(memory_space=pl.ANY))
    return pl.pallas_call(
        functools.partial(combine_kernel, count),
        grid=(rows // tile,),
        in_specs=in_specs,
        out_specs=pl.BlockSpec((None, tile, cols), lambda i: (side, i, 0)),
        out_shape=jax.ShapeDtypeStruct((2, rows, cols), jnp.float32),
        input_output_aliases=aliases,
        cost_estimate=pl.CostEstimate(
            flops=(2 + count) * rows * cols, bytes_accessed=(8 + 2 * count) * rows * cols, transcendentals=0
        ),
        compiler_params=pltpu.CompilerParams(dimension_semantics=("arbitrary",)),
    )(*operands)


MESH = pl.DeviceIdType.MESH
LANES = 128
SLOTS = 10
SENDS = 3
LAG = 3
BLOCKS = 4
SPLIT = 2
STEP = 128
RAW = 8


def line_kernel(n, nrow, halves, spectrum_in, wanted_in, fraction_in, out, scale, spectrum, wanted, fraction, own, par, cauchy, total, got, send, square,
                squares, values, spots, shares, ends, edge, seams, near_seams, raw, extra, table, pieces, lines, wide, roots, in_sem, own_sem, end_sem,
                par_send, par_got, send_sem, got_sem, square_send, square_got, value_send, value_got, spot_send,
                spot_got, share_send, share_got, edge_send, edge_got, near_send, near_got, raw_send,
                raw_got, free):
    c = lax.axis_index("col")
    d = lax.axis_index("depth")
    r = lax.axis_index("row")
    inner = cauchy.shape[1]
    half = inner // 2
    rows = own.shape[1]
    cols = cauchy.shape[2]
    tile = rows // BLOCKS
    blocks = 2 * BLOCKS
    chunks = blocks * SPLIT
    few = raw.shape[1]
    keep = tile - few
    inward = c + 1 - 2 * (c // (n - 1))
    outward = c - 1 + 2 * (c // (n - 2))
    last = (c == 0) | (c == n - 1)
    next_to_last = (c == 1) | (c == n - 2)
    groups = half // LANES
    shift_bits = half.bit_length() - 1
    place = 2 * c + d

    def part(b):
        return b // BLOCKS, pl.ds(pl.multiple_of((b % BLOCKS) * tile, tile), tile)

    def own_copy(b):
        side, where = part(b)
        return pltpu.make_async_copy(halves.at[side, where], own.at[side, where], own_sem.at[b])

    def send_to(source, target, sent, arrived, device):
        return pltpu.make_async_remote_copy(
            src_ref=source,
            dst_ref=target,
            send_sem=sent,
            recv_sem=arrived,
            device_id=device,
            device_id_type=MESH,
        )

    def par_copy(b):
        side, where = part(b)
        return send_to(
            halves.at[side, where], par.at[side, where], par_send.at[b], par_got.at[b], {"depth": 1 - d}
        )

    def square_copy(source, target):
        return send_to(
            square.at[target], squares.at[source], square_send.at[target], square_got.at[source], {"col": target}
        )

    def value_copy(source, target):
        return send_to(
            spectrum, values.at[source], value_send.at[target], value_got.at[source],
            {"col": target // 2, "depth": target % 2},
        )

    def spot_copy(source, target):
        return send_to(wanted, spots.at[source], spot_send.at[target], spot_got.at[source], {"col": target})

    def share_copy(source, target):
        return send_to(fraction, shares.at[source], share_send.at[target], share_got.at[source], {"col": target})

    def raw_copy():
        return send_to(
            halves.at[0, pl.ds(rows - few, few)], raw.at[0], raw_send.at[0], raw_got.at[0], {"col": inward}
        )

    def raw_pass():
        return send_to(raw.at[0], raw.at[1], raw_send.at[1], raw_got.at[1], {"depth": 1 - d})

    def near_copy(k):
        return send_to(seams.at[k, 0], near_seams.at[k], near_send.at[k], near_got.at[k], {"col": inward})

    def end_copy(side):
        at = (rows - 1 if side == 0 else 0) // 8 * 8
        return pltpu.make_async_copy(halves.at[side, pl.ds(at, 8)], ends.at[side], end_sem.at[side])

    step = math.gcd(inner, STEP)

    def edge_copy(side, k, source, target):
        return send_to(
            edge.at[side], seams.at[source, side], edge_send.at[side, k], edge_got.at[source, side],
            {"row": target // 2, "depth": target % 2},
        )

    def each(count, act):
        def one(b, carry):
            act(b)
            return carry

        lax.fori_loop(0, count, one, 0)

    barrier = pltpu.get_barrier_semaphore()
    for k in range(1, 2 * n):
        other = (place + k) % (2 * n)
        pl.semaphore_signal(
            barrier, inc=1, device_id={"col": other // 2, "depth": other % 2}, device_id_type=MESH
        )
    for k in range(1, nrow):
        for depth in range(2):
            pl.semaphore_signal(
                barrier, inc=1, device_id={"row": (r + k) % nrow, "depth": depth}, device_id_type=MESH
            )

    loads = [
        pltpu.make_async_copy(source, target, in_sem.at[k])
        for k, (source, target) in enumerate(
            ((spectrum_in, spectrum), (wanted_in, wanted), (fraction_in, fraction))
        )
    ]
    for side in range(2):
        end_copy(side).start()
    for load in loads:
        load.start()
    each(blocks, lambda b: own_copy(b).start())
    for load in loads:
        load.wait()
    for side in range(2):
        end_copy(side).wait()
        at = (rows - 1 if side == 0 else 0) % 8

        @pl.when(r == (nrow - 1 if side == 0 else 0))
        def _():
            line = ends[side].astype(jnp.float32)[at : at + 1, :]
            for j in range(groups):
                edge[side, j : j + 1, :] = line[:, j * LANES : (j + 1) * LANES]

    pl.semaphore_wait(barrier, 2 * n - 1 + 2 * (nrow - 1))

    for gone in range(n - 1, 0, -1):
        for other in (c + gone, c - gone):

            @pl.when((other >= 0) & (other < n))
            def _():
                spot_copy(c, other).start()
                share_copy(c, other).start()
                for depth in range(2):
                    value_copy(place, 2 * other + depth).start()

    value_copy(place, 2 * c + 1 - d).start()
    for side in range(2):

        @pl.when(r == (nrow - 1 if side == 0 else 0))
        def _():
            for k in range(1, 2 * nrow):
                edge_copy(side, k, d, (2 * r + d + k) % (2 * nrow)).start()
            seams[d, side] = edge[side]

    @pl.when(last)
    def _():
        raw_copy().start()

    each(blocks, lambda b: par_copy(b).start())
    values[place] = spectrum[...]
    spots[c] = wanted[...]
    shares[c] = fraction[...]

    for side in range(2):
        for near in range(2):
            source = d if near == 0 else 1 - d

            @pl.when((r != (nrow - 1 if side == 0 else 0)) | (near == 1))
            def _():
                edge_copy(side, 0, source, 2 * r + d).wait_recv()

    @pl.when(last)
    def _():
        for k in range(2):
            near_copy(k).start()

    for k in range(1, 2 * n):
        other = (place + k) % (2 * n)
        value_copy(other, place).wait_recv()
    for k in range(1, n):
        other = (c + k) % n
        spot_copy(other, c).wait_recv()
        share_copy(other, c).wait_recv()

    @pl.loop(0, 2 * n)
    def _(g):
        full = values[g]
        for side in range(2):
            for j in range(groups):
                table[pl.ds((g * 2 + side) * groups + j, 1), :] = full[side : side + 1, j * LANES : (j + 1) * LANES]

    for side in range(2):
        turned = []
        for near in range(2):
            source = d if near == 0 else 1 - d
            at = pl.multiple_of(((2 * c + source) * 2 + side) * groups, groups)
            turned.append(table[pl.ds(at, groups), :])
            turned.append(seams[source, side])
        lines[side] = jnp.concatenate(turned, axis=0).T

    flipped = table[...].T
    high = flipped.astype(jnp.bfloat16)
    rest = flipped - high.astype(jnp.float32)
    middle = rest.astype(jnp.bfloat16)
    low = (rest - middle.astype(jnp.float32)).astype(jnp.bfloat16)
    pieces[0:LANES, :] = high
    pieces[LANES : 2 * LANES, :] = middle
    pieces[2 * LANES : 3 * LANES, :] = low

    def widen(which, side):
        full = lines[which]
        for near in range(2):
            for kind in range(2):
                for j in range(groups):
                    column = (near * 2 + kind) * groups + j
                    at = (near * groups + j) * LANES
                    wide[kind, side, at : at + LANES, :] = jnp.broadcast_to(
                        full[:, column : column + 1], (LANES, LANES)
                    )

    def find_roots(way, target, piece):
        tall = cols // LANES
        begin = d * SPLIT + piece

        def choose(ref):
            full = ref[target]
            choice = full[0:tall, :]
            for k in range(1, 2 * SPLIT):
                choice = jnp.where(begin == k, full[k * tall : (k + 1) * tall, :], choice)
            return choice

        chosen = choose(spots)
        weight = choose(shares)
        hits, lanes = [], []
        entry = lax.broadcasted_iota(jnp.int32, (table.shape[0], LANES), 0)
        for above in range(2):
            for q in range(tall):
                where = chosen[q : q + 1, :] + above
                index = where >> 1
                within = index & (half - 1)
                row = ((index >> shift_bits) * 2 + (where & 1)) * groups + (within >> (LANES.bit_length() - 1))
                hits.append(jnp.where(entry == row, 1.0, 0.0).astype(jnp.bfloat16))
                lanes.append(within & (LANES - 1))
        hit = jnp.concatenate(hits, axis=1)
        lane = jnp.concatenate(lanes, axis=1)
        found = jnp.dot(pieces[...], hit, preferred_element_type=jnp.float32)
        found = (found[0:LANES] + found[LANES : 2 * LANES]) + found[2 * LANES : 3 * LANES]
        entry = lax.broadcasted_iota(jnp.int32, found.shape, 0)
        found = jnp.sum(jnp.where(entry == lane, found, 0.0), axis=0, keepdims=True)
        lower = found[:, 0:cols]
        weights = jnp.concatenate([weight[q : q + 1, :] for q in range(tall)], axis=1)
        roots[way, piece, 0:1, :] = lower
        roots[way, piece, 1:2, :] = weights * (found[:, cols : 2 * cols] - lower)

    def fill_near(way, piece):
        def one(b, carry):
            at = pl.ds(pl.multiple_of(b * step, step), step)
            value = wide[0, 0, at, :]
            seam = wide[1, 0, at, :]
            for q in range(cols // LANES):
                lanes = slice(q * LANES, (q + 1) * LANES)
                gap = (value - roots[way, piece, 0:1, lanes]) - roots[way, piece, 1:2, lanes]
                guess = pl.reciprocal(gap, approx=True)
                terms = (seam * guess) * (2.0 - gap * guess)
                cauchy[way, at, lanes] = terms.astype(jnp.bfloat16)
            return carry

        lax.fori_loop(0, inner // step, one, 0)

    def fill(way, side, piece, target, forward):
        @pl.when(side == 0)
        def _():
            find_roots(way, target, piece)

        def one(b, tallies):
            at = pl.ds(pl.multiple_of(b * step, step), step)
            value = wide[0, side, at, :]
            seam = wide[1, side, at, :]
            sums = []
            for q in range(cols // LANES):
                lanes = slice(q * LANES, (q + 1) * LANES)
                gap = (value - roots[way, piece, 0:1, lanes]) - roots[way, piece, 1:2, lanes]
                guess = pl.reciprocal(gap, approx=True)
                terms = (seam * guess) * (2.0 - gap * guess)
                cauchy[way, at, lanes] = terms.astype(jnp.bfloat16)
                terms = terms * terms
                tally = tallies[q]
                for j in range(step // 8):
                    tally = tally + terms[8 * j : 8 * j + 8, :]
                sums.append(tally)
            return tuple(sums)

        zero = jnp.zeros((8, LANES), jnp.float32)
        tallies = lax.fori_loop(0, inner // step, one, (zero,) * (cols // LANES))
        tally = jnp.concatenate(tallies, axis=1)

        @pl.when(side == 0)
        def _():
            square[target, piece] = tally

        @pl.when(side == 1)
        def _():
            square[target, piece] = square[target, piece] + tally

        @pl.when((side == 1) & (piece == SPLIT - 1) & forward)
        def _():
            square_copy(c, target).start()

    def item(q, carry):
        s = q // 2
        way = q % 2
        far = c + way * (n - 1 - 2 * c)
        t = s - LAG * far
        u = t // chunks
        i = t - u * chunks
        side = i // (BLOCKS * SPLIT)
        piece = (i // BLOCKS) % SPLIT
        where = pl.ds(pl.multiple_of((i % BLOCKS) * tile, tile), tile)
        held = pl.ds(pl.multiple_of(piece * cols, cols), cols)
        mark = n - 1 - u
        target = mark + way * (n - 1 - 2 * mark)
        valid = (t >= 0) & (t < jnp.minimum(n - far, n - 1) * chunks)
        forward = valid & (mark > far)
        arrive = valid & (mark == far)
        first = arrive & (2 * far > n - 1)
        later = arrive & (2 * far <= n - 1)
        dot = forward | first
        incoming = valid & (far > 0)
        slot = t % SLOTS
        spot = t % SENDS

        def line_copy(at, short=False):
            span = pl.ds(0, keep if short else tile)
            return send_to(
                send.at[way, at % SENDS, span], got.at[way, at % SLOTS, span], send_sem.at[way, at % SENDS],
                got_sem.at[way, at % SLOTS], {"col": c + 1 - 2 * way},
            )

        def partial(at):
            return (at % chunks < BLOCKS * SPLIT) & (at % BLOCKS == BLOCKS - 1)

        short_in = incoming & (far == 1) & partial(t)

        @pl.when((way == 0) & (s < 2))
        def _():
            widen(s, s)

        @pl.when((way == 0) & (s < chunks) & (s % (BLOCKS * SPLIT) < BLOCKS))
        def _():
            b = s // (BLOCKS * SPLIT) * BLOCKS + s % BLOCKS
            own_copy(b).wait()
            par_copy(b).wait_recv()

        @pl.when((q == 2 * LAG - 4) & next_to_last)
        def _():
            raw_copy().wait_recv()
            raw_pass().start()
            turned = []
            for near in range(2):
                source = d if near == 0 else 1 - d
                near_copy(source).wait_recv()
                at = pl.multiple_of((2 * outward + source) * 2 * groups, groups)
                turned.append(table[pl.ds(at, groups), :])
                turned.append(near_seams[source])
            lines[2] = jnp.concatenate(turned, axis=0).T

        @pl.when((q == 2 * LAG) & next_to_last)
        def _():
            raw_pass().wait_recv()

        @pl.when(dot & (i % BLOCKS == 0))
        def _():
            fill(way, side, piece, target, forward)

        @pl.when(dot)
        def _():
            a = jnp.dot(own[side, where, :], cauchy[way, 0:half, :], preferred_element_type=jnp.float32)
            b = jnp.dot(par[side, where, :], cauchy[way, half:inner, :], preferred_element_type=jnp.float32)
            total[...] = a + b

        @pl.when(short_in)
        def _():
            find_roots(way, target, piece)

            def one(k, carry):
                widen(2 - 2 * k, 0)

                @pl.when(k == 0)
                def _():
                    fill_near(way, piece)
                    a = jnp.dot(raw[0], cauchy[way, 0:half, :], preferred_element_type=jnp.float32)
                    b = jnp.dot(raw[1], cauchy[way, half:inner, :], preferred_element_type=jnp.float32)
                    extra[...] = a + b

                return carry

            lax.fori_loop(0, 2, one, 0)
            line_copy(t, True).wait_recv()
            got[way, slot, keep:tile, :] = extra[...].astype(jnp.bfloat16)

        @pl.when(incoming & jnp.logical_not(short_in))
        def _():
            line_copy(t).wait_recv()

        before = (far == 0) & partial(t - SENDS)

        @pl.when(forward & (t >= SENDS) & before)
        def _():
            line_copy(t - SENDS, True).wait_send()

        @pl.when(forward & (t >= SENDS) & jnp.logical_not(before))
        def _():
            line_copy(t - SENDS).wait_send()

        @pl.when(forward & (far == 0))
        def _():
            send[way, spot] = total[...].astype(jnp.bfloat16)

        @pl.when(forward & (far > 0))
        def _():
            send[way, spot] = (total[...] + got[way, slot].astype(jnp.float32)).astype(jnp.bfloat16)

        @pl.when(first)
        def _():
            out[side, where, held] = total[...] + got[way, slot].astype(jnp.float32)

        @pl.when(later)
        def _():
            out[side, where, held] = out[side, where, held] + got[way, slot].astype(jnp.float32)

        @pl.when(incoming & (t + SLOTS < (n - far) * chunks))
        def _():
            pl.semaphore_signal(
                free.at[way], inc=1, device_id={"col": c - 1 + 2 * way}, device_id_type=MESH
            )

        @pl.when(forward)
        def _():
            @pl.when(t >= SLOTS)
            def _():
                pl.semaphore_wait(free.at[way], 1)

            short_out = (far == 0) & partial(t)

            @pl.when(short_out)
            def _():
                line_copy(t, True).start()

            @pl.when(jnp.logical_not(short_out))
            def _():
                line_copy(t).start()

        return carry

    steps = (n - 1) * chunks + LAG
    lax.fori_loop(0, 2 * steps, item, 0)

    for way in range(2):
        far = c + way * (n - 1 - 2 * c)

        @pl.when(far < n - 1)
        def _():
            for spot in range(SENDS):
                send_to(
                    send.at[way, spot], got.at[way, spot], send_sem.at[way, spot], got_sem.at[way, spot],
                    {"col": c + 1 - 2 * way},
                ).wait_send()

    @pl.when(last)
    def _():
        raw_copy().wait_send()
        for k in range(2):
            near_copy(k).wait_send()

    @pl.when(next_to_last)
    def _():
        raw_pass().wait_send()

    each(blocks, lambda b: par_copy(b).wait_send())
    for k in range(1, 2 * n):
        value_copy(place, (place + k) % (2 * n)).wait_send()
    for side in range(2):

        @pl.when(r == (nrow - 1 if side == 0 else 0))
        def _():
            for k in range(1, 2 * nrow):
                edge_copy(side, k, d, (2 * r + d + k) % (2 * nrow)).wait_send()

    sums = square[c]
    for k in range(1, n):
        other = (c + k) % n
        spot_copy(c, other).wait_send()
        share_copy(c, other).wait_send()
        square_copy(c, other).wait_send()
        square_copy(other, c).wait_recv()
        sums = sums + squares[other]
    for piece in range(SPLIT):
        total_square = jnp.sum(sums[piece], axis=0, keepdims=True)
        scale[:, piece * cols : (piece + 1) * cols] = 1.0 / jnp.sqrt(total_square)


def scale_kernel(total, scale, out, ready, sem):
    rows = ready.shape[1]
    per_side = total.shape[1] // rows
    count = 2 * per_side

    def put(k):
        where = pl.ds(pl.multiple_of((k % per_side) * rows, rows), rows)
        return pltpu.make_async_copy(ready.at[k % 4], out.at[k // per_side, where], sem.at[k % 4])

    @pl.loop(0, count)
    def _(k):
        @pl.when(k >= 4)
        def _():
            put(k - 4).wait()

        where = pl.ds(pl.multiple_of((k % per_side) * rows, rows), rows)
        ready[k % 4] = total[k // per_side, where, :] * scale[...]
        put(k).start()

    for k in range(count - 4, count):
        put(k).wait()


def rescale(total, scale):
    _, rows, cols = total.shape
    tile = rows // 8
    vmem = pl.BlockSpec(memory_space=pltpu.VMEM)
    return pl.pallas_call(
        scale_kernel,
        in_specs=[vmem, vmem],
        out_specs=pl.BlockSpec(memory_space=pl.ANY),
        out_shape=jax.ShapeDtypeStruct(total.shape, jnp.float32),
        scratch_shapes=[pltpu.VMEM((4, tile, cols), jnp.float32), pltpu.SemaphoreType.DMA((4,))],
        cost_estimate=pl.CostEstimate(
            flops=2 * rows * cols, bytes_accessed=16 * rows * cols, transcendentals=0
        ),
        compiler_params=pltpu.CompilerParams(vmem_limit_bytes=16 * 1024 * 1024),
    )(total, scale)


def line_product(n, nrow, halves, spectrum, wanted, fraction):
    _, rows, half = halves.shape
    kcol = wanted.shape[0]
    share = kcol // 2
    cols = share // SPLIT
    tile = rows // BLOCKS
    blocks = 2 * BLOCKS
    groups = half // LANES
    dma = pltpu.SemaphoreType.DMA
    vmem = pl.BlockSpec(memory_space=pltpu.VMEM)
    return pl.pallas_call(
        functools.partial(line_kernel, n, nrow),
        in_specs=[pl.BlockSpec(memory_space=pl.ANY)] * 4,
        out_specs=[vmem, vmem],
        out_shape=[
            pltpu.VMEM((2, rows, share), jnp.float32),
            pltpu.VMEM((1, share), jnp.float32),
        ],
        scratch_shapes=[
            pltpu.VMEM((2, half), jnp.float32),
            pltpu.VMEM((kcol // LANES, LANES), jnp.int32),
            pltpu.VMEM((kcol // LANES, LANES), jnp.float32),
            pltpu.VMEM((2, rows, half), jnp.bfloat16),
            pltpu.VMEM((2, rows, half), jnp.bfloat16),
            pltpu.VMEM((2, 2 * half, cols), jnp.bfloat16),
            pltpu.VMEM((tile, cols), jnp.float32),
            pltpu.VMEM((2, SLOTS, tile, cols), jnp.bfloat16),
            pltpu.VMEM((2, SENDS, tile, cols), jnp.bfloat16),
            pltpu.VMEM((n, SPLIT, 8, cols), jnp.float32),
            pltpu.VMEM((n, SPLIT, 8, cols), jnp.float32),
            pltpu.VMEM((2 * n, 2, half), jnp.float32),
            pltpu.VMEM((n, kcol // LANES, LANES), jnp.int32),
            pltpu.VMEM((n, kcol // LANES, LANES), jnp.float32),
            pltpu.VMEM((2, 8, half), jnp.bfloat16),
            pltpu.VMEM((2, groups, LANES), jnp.float32),
            pltpu.VMEM((2, 2, groups, LANES), jnp.float32),
            pltpu.VMEM((2, groups, LANES), jnp.float32),
            pltpu.VMEM((2, tile // RAW, half), jnp.bfloat16),
            pltpu.VMEM((tile // RAW, cols), jnp.float32),
            pltpu.VMEM((4 * n * groups, LANES), jnp.float32),
            pltpu.VMEM((3 * LANES, 4 * n * groups), jnp.bfloat16),
            pltpu.VMEM((3, LANES, 4 * groups), jnp.float32),
            pltpu.VMEM((2, 2, 2 * half, LANES), jnp.float32),
            pltpu.VMEM((2, SPLIT, 2, cols), jnp.float32),
            dma((3,)),
            dma((blocks,)),
            dma((2,)),
            dma((blocks,)),
            dma((blocks,)),
            dma((2, SENDS)),
            dma((2, SLOTS)),
            dma((n,)),
            dma((n,)),
            dma((2 * n,)),
            dma((2 * n,)),
            dma((n,)),
            dma((n,)),
            dma((n,)),
            dma((n,)),
            dma((2, 2 * nrow)),
            dma((2, 2)),
            dma((2,)),
            dma((2,)),
            dma((2,)),
            dma((2,)),
            pltpu.SemaphoreType.REGULAR((2,)),
        ],
        cost_estimate=pl.CostEstimate(
            flops=8 * n * rows * half * share,
            bytes_accessed=8 * rows * half + 8 * rows * share,
            transcendentals=4 * n * half * share,
        ),
        compiler_params=pltpu.CompilerParams(
            collective_id=0, has_side_effects=True, vmem_limit_bytes=55 * 1024 * 1024
        ),
    )(halves, spectrum, wanted.reshape(-1, LANES), fraction.reshape(-1, LANES))


def look_up(table, row, lane):
    pick = (row[:, None] == lax.broadcasted_iota(jnp.int32, (1, table.shape[0]), 1)).astype(jnp.float32)
    lines = jnp.dot(pick, table, precision=lax.Precision.HIGHEST, preferred_element_type=jnp.float32)
    lanes = lax.broadcasted_iota(jnp.int32, (1, table.shape[1]), 1)
    return jnp.sum(jnp.where(lane[:, None] == lanes, lines, 0.0), axis=1)


def body(halves, spectrum, wanted, fraction):
    ncols = lax.axis_size("col")
    ndepth = lax.axis_size("depth")
    nrow = lax.axis_size("row")
    col = lax.axis_index("col")
    layer = lax.axis_index("depth")
    rows_here = halves.shape[1]
    width_here = halves.shape[2]
    kcol = wanted.shape[0]
    share = kcol // ndepth

    if ncols == 4 and 8 * width_here == LANES * LANES:
        total, scale = line_product(ncols, nrow, halves, spectrum, wanted, fraction)
        return rescale(total, scale)

    edges = jnp.stack([halves[0, rows_here - 1], halves[1, 0]])
    edges = lax.all_gather(edges, "row", axis=0, tiled=False)
    seam = jnp.stack([edges[nrow - 1, 0], edges[0, 1]]).astype(jnp.float32)

    lanes = math.gcd(width_here, 128)
    flat = jnp.concatenate(
        [spectrum.reshape(-1), seam.reshape(-1), wanted.astype(jnp.float32), fraction]
    )
    flat = lax.all_gather(flat, ("col", "depth"), axis=0, tiled=False)
    pieces = jnp.split(flat, [2 * width_here, 4 * width_here, 4 * width_here + kcol], axis=1)
    values, seams, position, frac = pieces
    table = values.reshape(-1, lanes)
    position = position.reshape(ncols, ndepth, kcol)[:, 0]
    frac = frac.reshape(ncols, ndepth, kcol)[:, 0]
    position = lax.dynamic_slice_in_dim(position, layer * share, share, axis=1).reshape(-1).astype(jnp.int32)
    frac = lax.dynamic_slice_in_dim(frac, layer * share, share, axis=1)

    def ordered(where):
        index = where // 2
        within = index % width_here
        row = ((index // width_here) * 2 + where % 2) * (width_here // lanes) + within // lanes
        return look_up(table, row, within % lanes).reshape(ncols, share)

    lower = ordered(position)
    shift = frac * (ordered(position + 1) - lower)
    roots = jnp.stack([lower, shift], axis=1)

    def near(full):
        full = full.reshape(ncols, ndepth, 2, width_here)
        full = lax.dynamic_index_in_dim(full, col, 0, keepdims=False)
        full = jnp.where(layer == 0, full, full[::-1])
        return jnp.transpose(full, (1, 0, 2)).reshape(2, ndepth * width_here)

    lines = jnp.stack([near(values), near(seams)], axis=2)

    partner = lax.ppermute(halves, "depth", [(0, 1), (1, 0)])

    def step(chunk, dtype=jnp.bfloat16):
        mine = lax.dynamic_index_in_dim(roots, chunk, 0, keepdims=False)
        return [product(side, halves, partner, mine, lines, dtype) for side in range(2)]

    received = [[], []]
    for shift_by in range(1, ncols):
        parts = step((col + shift_by) % ncols)
        for side in range(2):
            moves = [(i, (i + shift_by) % ncols) for i in range(ncols)]
            received[side].append(lax.ppermute(parts[side], "col", moves))
    own = step(col, jnp.float32)
    last = own[1]

    mine = lax.dynamic_index_in_dim(roots, col, 0, keepdims=False)
    mine, _ = lax.optimization_barrier((mine, last))
    full_value = values.reshape(-1, 1)
    full_seam = seams.reshape(-1, 1)
    cauchy = full_seam / ((full_value - mine[0:1]) - mine[1:2])
    norms = jnp.sqrt(jnp.sum(cauchy * cauchy, axis=0, keepdims=True))

    out = combine(0, own[0], list(received[0]), norms, None)
    return combine(1, own[1], list(received[1]), norms, out)


def solution(mesh):
    in_specs = (P(None, "row", ("col", "depth")), P(None, ("col", "depth")), P("col"), P("col"))
    out_specs = P(None, "row", ("col", "depth"))
    return jax.shard_map(body, mesh=mesh, in_specs=in_specs, out_specs=out_specs, check_vma=False)
```

```python
import functools
import math

import jax
import jax.numpy as jnp
from jax import lax
from jax.experimental import pallas as pl
from jax.experimental.pallas import tpu as pltpu
from jax.sharding import PartitionSpec as P


def product_kernel(own_ref, par_ref, roots_ref, line_ref, out_ref, block_ref):
    inner = block_ref.shape[0]
    half = inner // 2
    step = math.gcd(inner, 64)

    @pl.when(pl.program_id(0) == 0)
    def _():
        lower = roots_ref[0:1, :]
        shift = roots_ref[1:2, :]

        def one(i, carry):
            rows = pl.ds(pl.multiple_of(i * step, step), step)
            value = line_ref[rows, 0:1]
            seam = line_ref[rows, 1:2]
            gap = (value - lower) - shift
            guess = pl.reciprocal(gap, approx=True)
            inverse = guess + guess * (1.0 - gap * guess)
            block_ref[rows, :] = (seam * inverse).astype(jnp.bfloat16)
            return carry

        lax.fori_loop(0, inner // step, one, 0)

    first = jnp.dot(own_ref[...], block_ref[0:half, :], preferred_element_type=jnp.float32)
    second = jnp.dot(par_ref[...], block_ref[half:inner, :], preferred_element_type=jnp.float32)
    out_ref[...] = (first + second).astype(out_ref.dtype)


def product(side, own, partner, roots, lines, dtype):
    rows = own.shape[1]
    half = own.shape[2]
    cols = roots.shape[1]
    tile = math.gcd(rows, 256)
    return pl.pallas_call(
        product_kernel,
        grid=(rows // tile,),
        in_specs=[
            pl.BlockSpec((None, tile, half), lambda i: (side, i, 0)),
            pl.BlockSpec((None, tile, half), lambda i: (side, i, 0)),
            pl.BlockSpec((2, cols), lambda i: (0, 0)),
            pl.BlockSpec((None, 2 * half, 2), lambda i: (side, 0, 0)),
        ],
        out_specs=pl.BlockSpec((tile, cols), lambda i: (i, 0)),
        out_shape=jax.ShapeDtypeStruct((rows, cols), dtype),
        scratch_shapes=[pltpu.VMEM((2 * half, cols), jnp.bfloat16)],
        cost_estimate=pl.CostEstimate(
            flops=4 * rows * half * cols,
            bytes_accessed=4 * rows * half + 4 * rows * cols,
            transcendentals=2 * half * cols,
        ),
        compiler_params=pltpu.CompilerParams(dimension_semantics=("arbitrary",)),
    )(own, partner, roots, lines)


def combine_kernel(count, *refs):
    own_ref = refs[0]
    norm_ref = refs[1 + count]
    out_ref = refs[-1]
    total = own_ref[...]
    for k in range(count):
        total = total + refs[1 + k][...].astype(jnp.float32)
    out_ref[...] = total / norm_ref[...]


def combine(side, own, parts, norms, whole):
    rows, cols = own.shape
    tile = math.gcd(rows, 256)
    count = len(parts)
    block = pl.BlockSpec((tile, cols), lambda i: (i, 0))
    operands = [own, *parts, norms]
    in_specs = [block] * (1 + count) + [pl.BlockSpec((1, cols), lambda i: (0, 0))]
    aliases = {}
    if whole is not None:
        aliases = {len(operands): 0}
        operands.append(whole)
        in_specs.append(pl.BlockSpec(memory_space=pl.ANY))
    return pl.pallas_call(
        functools.partial(combine_kernel, count),
        grid=(rows // tile,),
        in_specs=in_specs,
        out_specs=pl.BlockSpec((None, tile, cols), lambda i: (side, i, 0)),
        out_shape=jax.ShapeDtypeStruct((2, rows, cols), jnp.float32),
        input_output_aliases=aliases,
        cost_estimate=pl.CostEstimate(
            flops=(2 + count) * rows * cols, bytes_accessed=(8 + 2 * count) * rows * cols, transcendentals=0
        ),
        compiler_params=pltpu.CompilerParams(dimension_semantics=("arbitrary",)),
    )(*operands)


MESH = pl.DeviceIdType.MESH
LANES = 128
SLOTS = 10
SENDS = 3
LAG = 3
BLOCKS = 4
SPLIT = 2
STEP = 128
RAW = 8


def line_kernel(n, nrow, halves, spectrum_in, wanted_in, fraction_in, out, scale, spectrum, wanted, fraction, own, par, cauchy, total, got, send, square,
                squares, values, spots, shares, ends, edge, seams, near_seams, raw, extra, table, pieces, lines, wide, roots, in_sem, own_sem, end_sem,
                par_send, par_got, send_sem, got_sem, square_send, square_got, value_send, value_got, spot_send,
                spot_got, share_send, share_got, edge_send, edge_got, near_send, near_got, raw_send,
                raw_got, free):
    c = lax.axis_index("col")
    d = lax.axis_index("depth")
    r = lax.axis_index("row")
    inner = cauchy.shape[1]
    half = inner // 2
    rows = own.shape[1]
    cols = cauchy.shape[2]
    tile = rows // BLOCKS
    blocks = 2 * BLOCKS
    chunks = blocks * SPLIT
    few = raw.shape[1]
    keep = tile - few
    inward = c + 1 - 2 * (c // (n - 1))
    outward = c - 1 + 2 * (c // (n - 2))
    last = (c == 0) | (c == n - 1)
    next_to_last = (c == 1) | (c == n - 2)
    groups = half // LANES
    shift_bits = half.bit_length() - 1
    place = 2 * c + d

    def part(b):
        return b // BLOCKS, pl.ds(pl.multiple_of((b % BLOCKS) * tile, tile), tile)

    def own_copy(b):
        side, where = part(b)
        return pltpu.make_async_copy(halves.at[side, where], own.at[side, where], own_sem.at[b])

    def send_to(source, target, sent, arrived, device):
        return pltpu.make_async_remote_copy(
            src_ref=source,
            dst_ref=target,
            send_sem=sent,
            recv_sem=arrived,
            device_id=device,
            device_id_type=MESH,
        )

    def par_copy(b):
        side, where = part(b)
        return send_to(
            halves.at[side, where], par.at[side, where], par_send.at[b], par_got.at[b], {"depth": 1 - d}
        )

    def square_copy(source, target):
        return send_to(
            square.at[target], squares.at[source], square_send.at[target], square_got.at[source], {"col": target}
        )

    def value_copy(source, target):
        return send_to(
            spectrum, values.at[source], value_send.at[target], value_got.at[source],
            {"col": target // 2, "depth": target % 2},
        )

    def spot_copy(source, target):
        return send_to(wanted, spots.at[source], spot_send.at[target], spot_got.at[source], {"col": target})

    def share_copy(source, target):
        return send_to(fraction, shares.at[source], share_send.at[target], share_got.at[source], {"col": target})

    def raw_copy():
        return send_to(
            halves.at[0, pl.ds(rows - few, few)], raw.at[0], raw_send.at[0], raw_got.at[0], {"col": inward}
        )

    def raw_pass():
        return send_to(raw.at[0], raw.at[1], raw_send.at[1], raw_got.at[1], {"depth": 1 - d})

    def near_copy(k):
        return send_to(seams.at[k, 0], near_seams.at[k], near_send.at[k], near_got.at[k], {"col": inward})

    def end_copy(side):
        at = (rows - 1 if side == 0 else 0) // 8 * 8
        return pltpu.make_async_copy(halves.at[side, pl.ds(at, 8)], ends.at[side], end_sem.at[side])

    step = math.gcd(inner, STEP)

    def edge_copy(side, k, source, target):
        return send_to(
            edge.at[side], seams.at[source, side], edge_send.at[side, k], edge_got.at[source, side],
            {"row": target // 2, "depth": target % 2},
        )

    def each(count, act):
        def one(b, carry):
            act(b)
            return carry

        lax.fori_loop(0, count, one, 0)

    barrier = pltpu.get_barrier_semaphore()
    for k in range(1, 2 * n):
        other = (place + k) % (2 * n)
        pl.semaphore_signal(
            barrier, inc=1, device_id={"col": other // 2, "depth": other % 2}, device_id_type=MESH
        )
    for k in range(1, nrow):
        for depth in range(2):
            pl.semaphore_signal(
                barrier, inc=1, device_id={"row": (r + k) % nrow, "depth": depth}, device_id_type=MESH
            )

    loads = [
        pltpu.make_async_copy(source, target, in_sem.at[k])
        for k, (source, target) in enumerate(
            ((spectrum_in, spectrum), (wanted_in, wanted), (fraction_in, fraction))
        )
    ]
    for side in range(2):
        end_copy(side).start()
    for load in loads:
        load.start()
    each(blocks, lambda b: own_copy(b).start())
    for load in loads:
        load.wait()
    for side in range(2):
        end_copy(side).wait()
        at = (rows - 1 if side == 0 else 0) % 8

        @pl.when(r == (nrow - 1 if side == 0 else 0))
        def _():
            line = ends[side].astype(jnp.float32)[at : at + 1, :]
            for j in range(groups):
                edge[side, j : j + 1, :] = line[:, j * LANES : (j + 1) * LANES]

    pl.semaphore_wait(barrier, 2 * n - 1 + 2 * (nrow - 1))

    for gone in range(n - 1, 0, -1):
        for other in (c + gone, c - gone):

            @pl.when((other >= 0) & (other < n))
            def _():
                spot_copy(c, other).start()
                share_copy(c, other).start()
                for depth in range(2):
                    value_copy(place, 2 * other + depth).start()

    value_copy(place, 2 * c + 1 - d).start()
    for side in range(2):

        @pl.when(r == (nrow - 1 if side == 0 else 0))
        def _():
            for k in range(1, 2 * nrow):
                edge_copy(side, k, d, (2 * r + d + k) % (2 * nrow)).start()
            seams[d, side] = edge[side]

    @pl.when(last)
    def _():
        raw_copy().start()

    each(blocks, lambda b: par_copy(b).start())
    values[place] = spectrum[...]
    spots[c] = wanted[...]
    shares[c] = fraction[...]

    for side in range(2):
        for near in range(2):
            source = d if near == 0 else 1 - d

            @pl.when((r != (nrow - 1 if side == 0 else 0)) | (near == 1))
            def _():
                edge_copy(side, 0, source, 2 * r + d).wait_recv()

    @pl.when(last)
    def _():
        for k in range(2):
            near_copy(k).start()

    for k in range(1, 2 * n):
        other = (place + k) % (2 * n)
        value_copy(other, place).wait_recv()
    for k in range(1, n):
        other = (c + k) % n
        spot_copy(other, c).wait_recv()
        share_copy(other, c).wait_recv()

    @pl.loop(0, 2 * n)
    def _(g):
        full = values[g]
        for side in range(2):
            for j in range(groups):
                table[pl.ds((g * 2 + side) * groups + j, 1), :] = full[side : side + 1, j * LANES : (j + 1) * LANES]

    for side in range(2):
        turned = []
        for near in range(2):
            source = d if near == 0 else 1 - d
            at = pl.multiple_of(((2 * c + source) * 2 + side) * groups, groups)
            turned.append(table[pl.ds(at, groups), :])
            turned.append(seams[source, side])
        lines[side] = jnp.concatenate(turned, axis=0).T

    flipped = table[...].T
    high = flipped.astype(jnp.bfloat16)
    rest = flipped - high.astype(jnp.float32)
    middle = rest.astype(jnp.bfloat16)
    low = (rest - middle.astype(jnp.float32)).astype(jnp.bfloat16)
    pieces[0:LANES, :] = high
    pieces[LANES : 2 * LANES, :] = middle
    pieces[2 * LANES : 3 * LANES, :] = low

    def widen(which, side):
        full = lines[which]
        for near in range(2):
            for kind in range(2):
                for j in range(groups):
                    column = (near * 2 + kind) * groups + j
                    at = (near * groups + j) * LANES
                    wide[kind, side, at : at + LANES, :] = jnp.broadcast_to(
                        full[:, column : column + 1], (LANES, LANES)
                    )

    def find_roots(way, target, piece):
        tall = cols // LANES
        begin = d * SPLIT + piece

        def choose(ref):
            full = ref[target]
            choice = full[0:tall, :]
            for k in range(1, 2 * SPLIT):
                choice = jnp.where(begin == k, full[k * tall : (k + 1) * tall, :], choice)
            return choice

        chosen = choose(spots)
        weight = choose(shares)
        hits, lanes = [], []
        entry = lax.broadcasted_iota(jnp.int32, (table.shape[0], LANES), 0)
        for above in range(2):
            for q in range(tall):
                where = chosen[q : q + 1, :] + above
                index = where >> 1
                within = index & (half - 1)
                row = ((index >> shift_bits) * 2 + (where & 1)) * groups + (within >> (LANES.bit_length() - 1))
                hits.append(jnp.where(entry == row, 1.0, 0.0).astype(jnp.bfloat16))
                lanes.append(within & (LANES - 1))
        hit = jnp.concatenate(hits, axis=1)
        lane = jnp.concatenate(lanes, axis=1)
        found = jnp.dot(pieces[...], hit, preferred_element_type=jnp.float32)
        found = (found[0:LANES] + found[LANES : 2 * LANES]) + found[2 * LANES : 3 * LANES]
        entry = lax.broadcasted_iota(jnp.int32, found.shape, 0)
        found = jnp.sum(jnp.where(entry == lane, found, 0.0), axis=0, keepdims=True)
        lower = found[:, 0:cols]
        weights = jnp.concatenate([weight[q : q + 1, :] for q in range(tall)], axis=1)
        roots[way, piece, 0:1, :] = lower
        roots[way, piece, 1:2, :] = weights * (found[:, cols : 2 * cols] - lower)

    def fill_near(way, piece):
        def one(b, carry):
            at = pl.ds(pl.multiple_of(b * step, step), step)
            value = wide[0, 0, at, :]
            seam = wide[1, 0, at, :]
            for q in range(cols // LANES):
                lanes = slice(q * LANES, (q + 1) * LANES)
                gap = (value - roots[way, piece, 0:1, lanes]) - roots[way, piece, 1:2, lanes]
                guess = pl.reciprocal(gap, approx=True)
                terms = (seam * guess) * (2.0 - gap * guess)
                cauchy[way, at, lanes] = terms.astype(jnp.bfloat16)
            return carry

        lax.fori_loop(0, inner // step, one, 0)

    def fill(way, side, piece, target, forward):
        @pl.when(side == 0)
        def _():
            find_roots(way, target, piece)

        def one(b, tallies):
            at = pl.ds(pl.multiple_of(b * step, step), step)
            value = wide[0, side, at, :]
            seam = wide[1, side, at, :]
            sums = []
            for q in range(cols // LANES):
                lanes = slice(q * LANES, (q + 1) * LANES)
                gap = (value - roots[way, piece, 0:1, lanes]) - roots[way, piece, 1:2, lanes]
                guess = pl.reciprocal(gap, approx=True)
                terms = (seam * guess) * (2.0 - gap * guess)
                cauchy[way, at, lanes] = terms.astype(jnp.bfloat16)
                terms = terms * terms
                tally = tallies[q]
                for j in range(step // 8):
                    tally = tally + terms[8 * j : 8 * j + 8, :]
                sums.append(tally)
            return tuple(sums)

        zero = jnp.zeros((8, LANES), jnp.float32)
        tallies = lax.fori_loop(0, inner // step, one, (zero,) * (cols // LANES))
        tally = jnp.sum(jnp.concatenate(tallies, axis=1), axis=0, keepdims=True)

        @pl.when(side == 0)
        def _():
            square[target, piece] = tally

        @pl.when(side == 1)
        def _():
            square[target, piece] = square[target, piece] + tally

        @pl.when((side == 1) & (piece == SPLIT - 1) & forward)
        def _():
            square_copy(c, target).start()

    def finish():
        @pl.when(last)
        def _():
            raw_copy().wait_send()
            for k in range(2):
                near_copy(k).wait_send()

        @pl.when(next_to_last)
        def _():
            raw_pass().wait_send()

        each(blocks, lambda b: par_copy(b).wait_send())
        for k in range(1, 2 * n):
            value_copy(place, (place + k) % (2 * n)).wait_send()
        for side in range(2):

            @pl.when(r == (nrow - 1 if side == 0 else 0))
            def _():
                for k in range(1, 2 * nrow):
                    edge_copy(side, k, d, (2 * r + d + k) % (2 * nrow)).wait_send()

        sums = square[c]
        for k in range(1, n):
            other = (c + k) % n
            spot_copy(c, other).wait_send()
            share_copy(c, other).wait_send()
            square_copy(c, other).wait_send()
            square_copy(other, c).wait_recv()
            sums = sums + squares[other]
        for piece in range(SPLIT):
            scale[:, piece * cols : (piece + 1) * cols] = 1.0 / jnp.sqrt(sums[piece])

    steps = (n - 1) * chunks + LAG

    def item(q, carry):
        s = q // 2
        way = q % 2
        far = c + way * (n - 1 - 2 * c)
        t = s - LAG * far
        u = t // chunks
        i = t - u * chunks
        side = i // (BLOCKS * SPLIT)
        piece = (i // BLOCKS) % SPLIT
        where = pl.ds(pl.multiple_of((i % BLOCKS) * tile, tile), tile)
        held = pl.ds(pl.multiple_of(piece * cols, cols), cols)
        mark = n - 1 - u
        target = mark + way * (n - 1 - 2 * mark)
        valid = (t >= 0) & (t < jnp.minimum(n - far, n - 1) * chunks)
        forward = valid & (mark > far)
        arrive = valid & (mark == far)
        first = arrive & (2 * far > n - 1)
        later = arrive & (2 * far <= n - 1)
        dot = forward | first
        incoming = valid & (far > 0)
        slot = t % SLOTS
        spot = t % SENDS

        def line_copy(at, short=False):
            span = pl.ds(0, keep if short else tile)
            return send_to(
                send.at[way, at % SENDS, span], got.at[way, at % SLOTS, span], send_sem.at[way, at % SENDS],
                got_sem.at[way, at % SLOTS], {"col": c + 1 - 2 * way},
            )

        def partial(at):
            return (at % chunks < BLOCKS * SPLIT) & (at % BLOCKS == BLOCKS - 1)

        short_in = incoming & (far == 1) & partial(t)

        @pl.when(q == 2 * (steps - 1))
        def _():
            finish()

        @pl.when((way == 0) & (s < 2))
        def _():
            widen(s, s)

        @pl.when((way == 0) & (s < chunks) & (s % (BLOCKS * SPLIT) < BLOCKS))
        def _():
            b = s // (BLOCKS * SPLIT) * BLOCKS + s % BLOCKS
            own_copy(b).wait()
            par_copy(b).wait_recv()

        @pl.when((q == 2 * LAG - 4) & next_to_last)
        def _():
            raw_copy().wait_recv()
            raw_pass().start()
            turned = []
            for near in range(2):
                source = d if near == 0 else 1 - d
                near_copy(source).wait_recv()
                at = pl.multiple_of((2 * outward + source) * 2 * groups, groups)
                turned.append(table[pl.ds(at, groups), :])
                turned.append(near_seams[source])
            lines[2] = jnp.concatenate(turned, axis=0).T

        @pl.when((q == 2 * LAG) & next_to_last)
        def _():
            raw_pass().wait_recv()

        @pl.when(dot & (i % BLOCKS == 0))
        def _():
            fill(way, side, piece, target, forward)

        @pl.when(dot)
        def _():
            a = jnp.dot(own[side, where, :], cauchy[way, 0:half, :], preferred_element_type=jnp.float32)
            b = jnp.dot(par[side, where, :], cauchy[way, half:inner, :], preferred_element_type=jnp.float32)
            total[...] = a + b

        @pl.when(short_in)
        def _():
            find_roots(way, target, piece)

            def one(k, carry):
                widen(2 - 2 * k, 0)

                @pl.when(k == 0)
                def _():
                    fill_near(way, piece)
                    a = jnp.dot(raw[0], cauchy[way, 0:half, :], preferred_element_type=jnp.float32)
                    b = jnp.dot(raw[1], cauchy[way, half:inner, :], preferred_element_type=jnp.float32)
                    extra[...] = a + b

                return carry

            lax.fori_loop(0, 2, one, 0)
            line_copy(t, True).wait_recv()
            got[way, slot, keep:tile, :] = extra[...].astype(jnp.bfloat16)

        @pl.when(incoming & jnp.logical_not(short_in))
        def _():
            line_copy(t).wait_recv()

        before = (far == 0) & partial(t - SENDS)

        @pl.when(forward & (t >= SENDS) & before)
        def _():
            line_copy(t - SENDS, True).wait_send()

        @pl.when(forward & (t >= SENDS) & jnp.logical_not(before))
        def _():
            line_copy(t - SENDS).wait_send()

        @pl.when(forward & (far == 0))
        def _():
            send[way, spot] = total[...].astype(jnp.bfloat16)

        @pl.when(forward & (far > 0))
        def _():
            send[way, spot] = (total[...] + got[way, slot].astype(jnp.float32)).astype(jnp.bfloat16)

        @pl.when(first)
        def _():
            out[side, where, held] = total[...] + got[way, slot].astype(jnp.float32)

        @pl.when(later)
        def _():
            out[side, where, held] = out[side, where, held] + got[way, slot].astype(jnp.float32)

        @pl.when(incoming & (t + SLOTS < (n - far) * chunks))
        def _():
            pl.semaphore_signal(
                free.at[way], inc=1, device_id={"col": c - 1 + 2 * way}, device_id_type=MESH
            )

        @pl.when(forward)
        def _():
            @pl.when(t >= SLOTS)
            def _():
                pl.semaphore_wait(free.at[way], 1)

            short_out = (far == 0) & partial(t)

            @pl.when(short_out)
            def _():
                line_copy(t, True).start()

            @pl.when(jnp.logical_not(short_out))
            def _():
                line_copy(t).start()

        return carry

    lax.fori_loop(0, 2 * steps, item, 0)

    for way in range(2):
        far = c + way * (n - 1 - 2 * c)

        @pl.when(far < n - 1)
        def _():
            for spot in range(SENDS):
                send_to(
                    send.at[way, spot], got.at[way, spot], send_sem.at[way, spot], got_sem.at[way, spot],
                    {"col": c + 1 - 2 * way},
                ).wait_send()


def scale_kernel(total, scale, out, ready, sem):
    rows = ready.shape[1]
    per_side = total.shape[1] // rows
    count = 2 * per_side

    def put(k):
        where = pl.ds(pl.multiple_of((k % per_side) * rows, rows), rows)
        return pltpu.make_async_copy(ready.at[k % 4], out.at[k // per_side, where], sem.at[k % 4])

    @pl.loop(0, count)
    def _(k):
        @pl.when(k >= 4)
        def _():
            put(k - 4).wait()

        where = pl.ds(pl.multiple_of((k % per_side) * rows, rows), rows)
        ready[k % 4] = total[k // per_side, where, :] * scale[...]
        put(k).start()

    for k in range(count - 4, count):
        put(k).wait()


def rescale(total, scale):
    _, rows, cols = total.shape
    tile = rows // 8
    vmem = pl.BlockSpec(memory_space=pltpu.VMEM)
    return pl.pallas_call(
        scale_kernel,
        in_specs=[vmem, vmem],
        out_specs=pl.BlockSpec(memory_space=pl.ANY),
        out_shape=jax.ShapeDtypeStruct(total.shape, jnp.float32),
        scratch_shapes=[pltpu.VMEM((4, tile, cols), jnp.float32), pltpu.SemaphoreType.DMA((4,))],
        cost_estimate=pl.CostEstimate(
            flops=2 * rows * cols, bytes_accessed=16 * rows * cols, transcendentals=0
        ),
        compiler_params=pltpu.CompilerParams(vmem_limit_bytes=16 * 1024 * 1024),
    )(total, scale)


def line_product(n, nrow, halves, spectrum, wanted, fraction):
    _, rows, half = halves.shape
    kcol = wanted.shape[0]
    share = kcol // 2
    cols = share // SPLIT
    tile = rows // BLOCKS
    blocks = 2 * BLOCKS
    groups = half // LANES
    dma = pltpu.SemaphoreType.DMA
    vmem = pl.BlockSpec(memory_space=pltpu.VMEM)
    return pl.pallas_call(
        functools.partial(line_kernel, n, nrow),
        in_specs=[pl.BlockSpec(memory_space=pl.ANY)] * 4,
        out_specs=[vmem, vmem],
        out_shape=[
            pltpu.VMEM((2, rows, share), jnp.float32),
            pltpu.VMEM((1, share), jnp.float32),
        ],
        scratch_shapes=[
            pltpu.VMEM((2, half), jnp.float32),
            pltpu.VMEM((kcol // LANES, LANES), jnp.int32),
            pltpu.VMEM((kcol // LANES, LANES), jnp.float32),
            pltpu.VMEM((2, rows, half), jnp.bfloat16),
            pltpu.VMEM((2, rows, half), jnp.bfloat16),
            pltpu.VMEM((2, 2 * half, cols), jnp.bfloat16),
            pltpu.VMEM((tile, cols), jnp.float32),
            pltpu.VMEM((2, SLOTS, tile, cols), jnp.bfloat16),
            pltpu.VMEM((2, SENDS, tile, cols), jnp.bfloat16),
            pltpu.VMEM((n, SPLIT, 1, cols), jnp.float32),
            pltpu.VMEM((n, SPLIT, 1, cols), jnp.float32),
            pltpu.VMEM((2 * n, 2, half), jnp.float32),
            pltpu.VMEM((n, kcol // LANES, LANES), jnp.int32),
            pltpu.VMEM((n, kcol // LANES, LANES), jnp.float32),
            pltpu.VMEM((2, 8, half), jnp.bfloat16),
            pltpu.VMEM((2, groups, LANES), jnp.float32),
            pltpu.VMEM((2, 2, groups, LANES), jnp.float32),
            pltpu.VMEM((2, groups, LANES), jnp.float32),
            pltpu.VMEM((2, tile // RAW, half), jnp.bfloat16),
            pltpu.VMEM((tile // RAW, cols), jnp.float32),
            pltpu.VMEM((4 * n * groups, LANES), jnp.float32),
            pltpu.VMEM((3 * LANES, 4 * n * groups), jnp.bfloat16),
            pltpu.VMEM((3, LANES, 4 * groups), jnp.float32),
            pltpu.VMEM((2, 2, 2 * half, LANES), jnp.float32),
            pltpu.VMEM((2, SPLIT, 2, cols), jnp.float32),
            dma((3,)),
            dma((blocks,)),
            dma((2,)),
            dma((blocks,)),
            dma((blocks,)),
            dma((2, SENDS)),
            dma((2, SLOTS)),
            dma((n,)),
            dma((n,)),
            dma((2 * n,)),
            dma((2 * n,)),
            dma((n,)),
            dma((n,)),
            dma((n,)),
            dma((n,)),
            dma((2, 2 * nrow)),
            dma((2, 2)),
            dma((2,)),
            dma((2,)),
            dma((2,)),
            dma((2,)),
            pltpu.SemaphoreType.REGULAR((2,)),
        ],
        cost_estimate=pl.CostEstimate(
            flops=8 * n * rows * half * share,
            bytes_accessed=8 * rows * half + 8 * rows * share,
            transcendentals=4 * n * half * share,
        ),
        compiler_params=pltpu.CompilerParams(
            collective_id=0, has_side_effects=True, vmem_limit_bytes=55 * 1024 * 1024
        ),
    )(halves, spectrum, wanted.reshape(-1, LANES), fraction.reshape(-1, LANES))


def look_up(table, row, lane):
    pick = (row[:, None] == lax.broadcasted_iota(jnp.int32, (1, table.shape[0]), 1)).astype(jnp.float32)
    lines = jnp.dot(pick, table, precision=lax.Precision.HIGHEST, preferred_element_type=jnp.float32)
    lanes = lax.broadcasted_iota(jnp.int32, (1, table.shape[1]), 1)
    return jnp.sum(jnp.where(lane[:, None] == lanes, lines, 0.0), axis=1)


def body(halves, spectrum, wanted, fraction):
    ncols = lax.axis_size("col")
    ndepth = lax.axis_size("depth")
    nrow = lax.axis_size("row")
    col = lax.axis_index("col")
    layer = lax.axis_index("depth")
    rows_here = halves.shape[1]
    width_here = halves.shape[2]
    kcol = wanted.shape[0]
    share = kcol // ndepth

    if ncols == 4 and 8 * width_here == LANES * LANES:
        total, scale = line_product(ncols, nrow, halves, spectrum, wanted, fraction)
        return rescale(total, scale)

    edges = jnp.stack([halves[0, rows_here - 1], halves[1, 0]])
    edges = lax.all_gather(edges, "row", axis=0, tiled=False)
    seam = jnp.stack([edges[nrow - 1, 0], edges[0, 1]]).astype(jnp.float32)

    lanes = math.gcd(width_here, 128)
    flat = jnp.concatenate(
        [spectrum.reshape(-1), seam.reshape(-1), wanted.astype(jnp.float32), fraction]
    )
    flat = lax.all_gather(flat, ("col", "depth"), axis=0, tiled=False)
    pieces = jnp.split(flat, [2 * width_here, 4 * width_here, 4 * width_here + kcol], axis=1)
    values, seams, position, frac = pieces
    table = values.reshape(-1, lanes)
    position = position.reshape(ncols, ndepth, kcol)[:, 0]
    frac = frac.reshape(ncols, ndepth, kcol)[:, 0]
    position = lax.dynamic_slice_in_dim(position, layer * share, share, axis=1).reshape(-1).astype(jnp.int32)
    frac = lax.dynamic_slice_in_dim(frac, layer * share, share, axis=1)

    def ordered(where):
        index = where // 2
        within = index % width_here
        row = ((index // width_here) * 2 + where % 2) * (width_here // lanes) + within // lanes
        return look_up(table, row, within % lanes).reshape(ncols, share)

    lower = ordered(position)
    shift = frac * (ordered(position + 1) - lower)
    roots = jnp.stack([lower, shift], axis=1)

    def near(full):
        full = full.reshape(ncols, ndepth, 2, width_here)
        full = lax.dynamic_index_in_dim(full, col, 0, keepdims=False)
        full = jnp.where(layer == 0, full, full[::-1])
        return jnp.transpose(full, (1, 0, 2)).reshape(2, ndepth * width_here)

    lines = jnp.stack([near(values), near(seams)], axis=2)

    partner = lax.ppermute(halves, "depth", [(0, 1), (1, 0)])

    def step(chunk, dtype=jnp.bfloat16):
        mine = lax.dynamic_index_in_dim(roots, chunk, 0, keepdims=False)
        return [product(side, halves, partner, mine, lines, dtype) for side in range(2)]

    received = [[], []]
    for shift_by in range(1, ncols):
        parts = step((col + shift_by) % ncols)
        for side in range(2):
            moves = [(i, (i + shift_by) % ncols) for i in range(ncols)]
            received[side].append(lax.ppermute(parts[side], "col", moves))
    own = step(col, jnp.float32)
    last = own[1]

    mine = lax.dynamic_index_in_dim(roots, col, 0, keepdims=False)
    mine, _ = lax.optimization_barrier((mine, last))
    full_value = values.reshape(-1, 1)
    full_seam = seams.reshape(-1, 1)
    cauchy = full_seam / ((full_value - mine[0:1]) - mine[1:2])
    norms = jnp.sqrt(jnp.sum(cauchy * cauchy, axis=0, keepdims=True))

    out = combine(0, own[0], list(received[0]), norms, None)
    return combine(1, own[1], list(received[1]), norms, out)


def solution(mesh):
    in_specs = (P(None, "row", ("col", "depth")), P(None, ("col", "depth")), P("col"), P("col"))
    out_specs = P(None, "row", ("col", "depth"))
    return jax.shard_map(body, mesh=mesh, in_specs=in_specs, out_specs=out_specs, check_vma=False)
```
